8 devices in a mesh: dp: 1 (over z), tp: 8 (over y, x, core).
Axes of the slice: x: 2, y: 2, z: 1, core: 2. Of those that a mesh axis runs over, the one named last changes fastest.
Arguments:
- tokens_in: bfloat16 [32, 256, 1280], P('dp')
- ln_scale: bfloat16 [2, 1280], replicated
- w_query: bfloat16 [2, 1280, 1280], P(None, None, 'tp')
- w_key: bfloat16 [2, 1280, 1280], P(None, None, 'tp')
- w_value: bfloat16 [2, 1280, 1280], P(None, None, 'tp')
- q_scale: bfloat16 [2, 80], replicated
- k_scale: bfloat16 [2, 80], replicated
- w_out: bfloat16 [2, 1280, 1280], P(None, 'tp')
- b_out: bfloat16 [2, 1280], replicated
- w_up: bfloat16 [2, 1280, 5120], P(None, None, 'tp')
- b_up: bfloat16 [2, 5120], P(None, 'tp')
- w_down: bfloat16 [2, 5120, 1280], P(None, 'tp')
- b_down: bfloat16 [2, 1280], replicated
Outputs:
- output: bfloat16 [32, 256, 1280], P('dp')
All inputs are finite; a program needn't handle non-finite values.
Results may differ from the reference program's by a relative error of at most 0.0129673.
Values are sent between devices in bfloat16 or wider.
A program may use at most 1 GiB of HBM per device.

```python
import jax
import jax.numpy as jnp
from jax import lax

IMAGES = 32
SEQ_LEN = 256
MODEL_DIM = 1280
NUM_HEADS = 16
HEAD_DIM = 80
MLP_DIM = 5120
LAYERS = 2
LN_EPS = 1e-6


def setup_inputs(seed: int = 0, part: int = 0) -> dict:
    base_key = jax.random.key(seed)
    part_key = jax.random.fold_in(base_key, part)
    key_list = jax.random.split(base_key, 12)
    hidden = NUM_HEADS * HEAD_DIM

    def normal(rng_key, arr_shape, spread, offset):
        std_draw = jax.random.normal(rng_key, arr_shape, jnp.float32)
        return (offset + spread * std_draw).astype(jnp.bfloat16)

    return {
        "tokens_in": normal(part_key, (IMAGES, SEQ_LEN, MODEL_DIM), 1.0, 0.0),
        "ln_scale": normal(key_list[0], (LAYERS, MODEL_DIM), 0.3, 1.0),
        "w_query": normal(key_list[1], (LAYERS, MODEL_DIM, hidden), MODEL_DIM ** -0.5, 0.0),
        "w_key": normal(key_list[2], (LAYERS, MODEL_DIM, hidden), MODEL_DIM ** -0.5, 0.0),
        "w_value": normal(key_list[3], (LAYERS, MODEL_DIM, hidden), MODEL_DIM ** -0.5, 0.0),
        "q_scale": normal(key_list[4], (LAYERS, HEAD_DIM), 0.3, 1.5),
        "k_scale": normal(key_list[5], (LAYERS, HEAD_DIM), 0.3, 1.5),
        "w_out": normal(key_list[6], (LAYERS, hidden, MODEL_DIM), hidden ** -0.5, 0.0),
        "b_out": normal(key_list[7], (LAYERS, MODEL_DIM), 0.5, 0.0),
        "w_up": normal(key_list[8], (LAYERS, MODEL_DIM, MLP_DIM), MODEL_DIM ** -0.5, 0.0),
        "b_up": normal(key_list[9], (LAYERS, MLP_DIM), 0.5, 0.0),
        "w_down": normal(key_list[10], (LAYERS, MLP_DIM, MODEL_DIM), MLP_DIM ** -0.5, 0.0),
        "b_down": normal(key_list[11], (LAYERS, MODEL_DIM), 0.5, 0.0),
    }


def layer_norm(values, scale_vec):
    mean_val = jnp.mean(values, axis=-1, keepdims=True)
    centered = values - mean_val
    variance = jnp.mean(centered * centered, axis=-1, keepdims=True)
    return centered * lax.rsqrt(variance + LN_EPS) * scale_vec.astype(jnp.float32)


def one_layer(tokens_in, ln_scale, w_query, w_key, w_value, q_scale, k_scale, w_out, b_out, w_up, b_up, w_down, b_down):
    n_tokens = IMAGES * SEQ_LEN
    residual = tokens_in.reshape(n_tokens, MODEL_DIM).astype(jnp.float32)
    normed = layer_norm(residual, ln_scale).astype(jnp.bfloat16)

    def project(weight):
        projected = jnp.dot(normed, weight, preferred_element_type=jnp.float32)
        return projected.reshape(IMAGES, SEQ_LEN, NUM_HEADS, HEAD_DIM)

    queries = layer_norm(project(w_query), q_scale).astype(jnp.bfloat16)
    keys_all = layer_norm(project(w_key), k_scale).astype(jnp.bfloat16)
    values_all = project(w_value).astype(jnp.bfloat16)

    def attend(operands):
        q_img, k_img, v_img = operands
        scores = jnp.einsum("qhd,khd->hqk", q_img.astype(jnp.float32), k_img.astype(jnp.float32)) * HEAD_DIM ** -0.5
        attn_prob = jax.nn.softmax(scores, axis=-1).astype(jnp.bfloat16)
        mixed_val = jnp.einsum("hqk,khd->qhd", attn_prob.astype(jnp.float32), v_img.astype(jnp.float32))
        return mixed_val.astype(jnp.bfloat16)

    attended = lax.map(attend, (queries, keys_all, values_all)).reshape(n_tokens, NUM_HEADS * HEAD_DIM)
    attn_part = jnp.dot(attended, w_out, preferred_element_type=jnp.float32)
    pre_act = jnp.dot(normed, w_up, preferred_element_type=jnp.float32) + b_up.astype(jnp.float32)
    activated = jax.nn.gelu(pre_act, approximate=True).astype(jnp.bfloat16)
    mlp_part = jnp.dot(activated, w_down, preferred_element_type=jnp.float32)
    summed = residual + b_out.astype(jnp.float32) + b_down.astype(jnp.float32) + attn_part + mlp_part
    return summed.astype(jnp.bfloat16).reshape(IMAGES, SEQ_LEN, MODEL_DIM)


def reference(tokens_in, ln_scale, w_query, w_key, w_value, q_scale, k_scale, w_out, b_out, w_up, b_up, w_down, b_down):
    def step_fn(state_in, params):
        return one_layer(state_in, *params), None

    encoded, _ = lax.scan(step_fn, tokens_in, (ln_scale, w_query, w_key, w_value, q_scale, k_scale, w_out, b_out, w_up, b_up, w_down, b_down))
    return encoded
```

```python
import jax
import jax.numpy as jnp
from jax import lax
from jax.experimental import pallas as pl
from jax.experimental.pallas import tpu as pltpu
from jax.sharding import PartitionSpec as P

LN_EPS = 1e-6
MESH = pl.DeviceIdType.MESH
F32, BF16 = jnp.float32, jnp.bfloat16

IMGS = 8
OWN = 4
SPLIT = 384
PIECES = 8


def normalize(values):
    mean_val = jnp.mean(values, axis=-1, keepdims=True)
    centered = values - mean_val
    variance = jnp.mean(centered * centered, axis=-1, keepdims=True)
    return centered * lax.rsqrt(variance + LN_EPS)


def gelu(pre):
    inner = (2.0 / jnp.pi) ** 0.5 * (pre + 0.044715 * (pre * pre * pre))
    return pre * (0.5 * (1.0 + jnp.tanh(inner)))


def dot(lhs, rhs):
    return jnp.dot(lhs, rhs, preferred_element_type=F32)


def fused(
    tok, wq, wk, wv, wo, w1, w2, ln, qs, ks, bo, bu, b2,
    out, gq, go, g1, g2,
    vq, vo, v1, v2, vb, gain, acc, hid, x1, snd0, rcv0, snd1, rcv1, fin,
    loc0, loc1, xs, s_b, r_b,
    s_c0, r_c0, s_x0, r_x0, s_f0, r_f0,
    s_c1, r_c1, s_y1, r_y1, s_f1, r_f1,
    s_p0, r_p0, s_g0, r_g0, s_p1, r_p1,
    s_out, s_oc, r_oc, s_ox, r_ox, s_oy, r_oy, s_od, r_od,
    s_ex, r_ex, s_ey, r_ey, s_ed, r_ed,
):
    seq, dim = hid.shape[1], hid.shape[2]
    heads_w = wo.shape[1]
    head_dim = qs.shape[1]
    n_heads = heads_w // head_dim
    mlp = w1.shape[2]
    me = lax.axis_index("tp")
    y = me // 4
    x = (me // 2) % 2
    c = me % 2
    cp = me + 1 - 2 * c
    xp = me + 2 - 4 * x
    yp = me + 4 - 8 * y
    xc = xp + 1 - 2 * c
    yc = yp + 1 - 2 * c

    def remote(src, dst, send, recv, dev):
        return pltpu.make_async_remote_copy(
            src_ref=src, dst_ref=dst, send_sem=send, recv_sem=recv,
            device_id={"tp": dev}, device_id_type=MESH)

    def pieces_of(layer):
        return (
            wq.at[layer], wk.at[layer], wv.at[layer], wo.at[layer],
            w1.at[layer, :, pl.ds(0, SPLIT)], w2.at[layer, pl.ds(0, SPLIT), :],
            w1.at[layer, :, pl.ds(SPLIT, mlp - SPLIT)], w2.at[layer, pl.ds(SPLIT, mlp - SPLIT), :],
        )

    def slot_of(refs, slot):
        a, b, d, e = refs
        third = [a.at[slot, pl.ds(n * heads_w, heads_w), :] for n in range(3)]
        return (
            *third, b.at[slot],
            d.at[slot, :, pl.ds(0, SPLIT)], e.at[slot, pl.ds(0, SPLIT), :],
            d.at[slot, :, pl.ds(SPLIT, mlp - SPLIT)], e.at[slot, pl.ds(SPLIT, mlp - SPLIT), :],
        )

    vmem = (vq, vo, v1, v2)
    land = (gq, go, g1, g2)

    def moves(src, dst, send, recv, dev):
        return [remote(src[q], dst[q], send.at[q], recv.at[q], dev) for q in range(PIECES)]

    own_load = [pltpu.make_async_copy(pieces_of(0)[q], slot_of(vmem, 0)[q], loc0.at[q]) for q in range(PIECES)]
    own_core = moves(pieces_of(0), slot_of(vmem, 1), s_c0, r_c0, cp)
    own_x = moves(pieces_of(0), slot_of(vmem, 2), s_x0, r_x0, xp)
    fwd_x = moves(slot_of(vmem, 2), slot_of(vmem, 3), s_f0, r_f0, cp)
    nxt_core = moves(pieces_of(1), slot_of(land, 0), s_c1, r_c1, cp)
    nxt_y = moves(pieces_of(1), slot_of(land, 1), s_y1, r_y1, yp)
    fwd_y = moves(slot_of(land, 1), slot_of(land, 2), s_f1, r_f1, cp)
    peers = (cp, xp, xc, yp, yc)
    biases = [remote(bu, vb.at[n + 1], s_b.at[n], r_b.at[n], peers[n]) for n in range(5)]

    def nxt_load(slot, q):
        src = pieces_of(1) if slot == 0 else slot_of(land, slot - 1)
        return pltpu.make_async_copy(src[q], slot_of(vmem, slot)[q], loc1.at[slot, q])

    group = (2 * x + c) * IMGS

    def image_of(i):
        far = (i < OWN).astype(jnp.int32) if not isinstance(i, int) else int(i < OWN)
        return group + OWN * (y + far - 2 * y * far) + i % OWN

    def load_x(i):
        return pltpu.make_async_copy(tok.at[pl.ds(image_of(i) * seq, seq), :], hid.at[i], xs.at[i])

    for q in range(PIECES):
        own_load[q].start()
    for i in range(IMGS):
        load_x(i).start()

    barrier = pltpu.get_barrier_semaphore()
    for dev in peers:
        pl.semaphore_signal(barrier, inc=1, device_id={"tp": dev}, device_id_type=MESH)
    pl.semaphore_wait(barrier, len(peers))

    for copy in biases:
        copy.start()
    for q in range(PIECES):
        own_x[q].start()
        nxt_y[q].start()
        own_core[q].start()
    for q in range(PIECES):
        nxt_core[q].start()

    def row(ref, layer):
        return ref[layer : layer + 1, :].astype(F32)

    vb[0] = bu[...]
    for layer in range(2):
        for n, ref in enumerate((qs, ks)):
            gain[layer, n] = jnp.broadcast_to(row(ref, layer), (seq, head_dim)).T

    def head_norm(values, layer, n):
        mean_val = jnp.mean(values, axis=0, keepdims=True)
        centered = values - mean_val
        variance = jnp.mean(centered * centered, axis=0, keepdims=True)
        return centered * lax.rsqrt(variance + LN_EPS) * gain[layer, n]

    def attend(i, slot, layer):
        proj = lax.dot_general(vq[slot], hid[i], (((1,), (1,)), ((), ())), preferred_element_type=F32)
        mixed = []
        for hd in range(n_heads):
            lo = hd * head_dim
            q_h = head_norm(proj[lo : lo + head_dim], layer, 0).astype(BF16)
            k_h = head_norm(proj[heads_w + lo : heads_w + lo + head_dim], layer, 1).T.astype(BF16)
            v_h = proj[2 * heads_w + lo : 2 * heads_w + lo + head_dim].astype(BF16)
            scores = dot(k_h, q_h) * head_dim ** -0.5
            weight = jnp.exp(scores - jnp.max(scores, axis=0, keepdims=True))
            total = jnp.sum(weight, axis=0, keepdims=True)
            prob = (weight * (1.0 / total)).astype(BF16)
            mixed.append(dot(v_h, prob))
        mix = jnp.concatenate(mixed, axis=0).T.astype(BF16)
        return dot(mix, vo[slot])

    def mlp_part(i, slot, layer, lo, hi):
        bias = vb[slot + 2 * layer * (slot // 2), layer : layer + 1, lo:hi].astype(F32)
        act = gelu(dot(hid[i], v1[slot, :, lo:hi]) + bias).astype(BF16)
        return dot(act, v2[slot, lo:hi, :])

    @pl.loop(0, IMGS)
    def _(i):
        load_x(i).wait()
        values = hid[i].astype(F32)
        hid[i] = (normalize(values) * row(ln, 0)).astype(BF16)

        @pl.when(i < OWN)
        def _():
            acc[i] = jnp.zeros((seq, dim), F32)

        @pl.when(i >= OWN)
        def _():
            acc[i] = values + row(bo, 0) + row(b2, 0)

    @pl.loop(0, 2)
    def _(slot):
        @pl.when(slot == 0)
        def _():
            for q in range(PIECES):
                own_load[q].wait()
            for copy in biases:
                copy.wait_recv()

        @pl.when(slot == 1)
        def _():
            for q in range(PIECES):
                own_core[q].wait_recv()

        @pl.loop(0, IMGS)
        def _(i):
            acc[i] += attend(i, slot, 0) + mlp_part(i, slot, 0, 0, mlp)

    for q in range(PIECES):
        nxt_core[q].wait_recv()
    for q in range(PIECES):
        nxt_load(0, q).start()
        nxt_load(1, q).start()

    def arrive(slot, pieces):
        @pl.when(slot == 2)
        def _():
            for q in pieces:
                own_x[q].wait_recv()
                fwd_x[q].start()

        @pl.when(slot == 3)
        def _():
            for q in pieces:
                fwd_x[q].wait_recv()

    @pl.loop(2, 4)
    def _(slot):
        arrive(slot, (0, 1, 2, 3))

        @pl.loop(0, IMGS)
        def _(i):
            acc[i] += attend(i, slot, 0)

    @pl.loop(2, 4)
    def _(slot):
        arrive(slot, (4, 5))

        @pl.loop(0, IMGS)
        def _(i):
            acc[i] += mlp_part(i, slot, 0, 0, SPLIT)

    for q in (6, 7):
        own_x[q].wait_recv()
        fwd_x[q].start()
    for q in (6, 7):
        fwd_x[q].wait_recv()

    def part0(k):
        return remote(snd0.at[k], rcv0.at[k], s_p0.at[k], r_p0.at[k], yp)

    def give0(k):
        return remote(x1.at[k], x1.at[OWN + k], s_g0.at[k], r_g0.at[k], xp)

    def part1(k):
        return remote(snd1.at[k], rcv1.at[k], s_p1.at[k], r_p1.at[k], xp)

    @pl.loop(0, IMGS)
    def _(i):
        acc[i] += mlp_part(i, 2, 0, SPLIT, mlp) + mlp_part(i, 3, 0, SPLIT, mlp)

        @pl.when(i < OWN)
        def _():
            snd0[i] = acc[i].astype(BF16)
            part0(i).start()

    for q in range(PIECES):
        nxt_y[q].wait_recv()
        fwd_y[q].start()
    for q in range(PIECES):
        fwd_x[q].wait_send()
    for q in range(PIECES):
        nxt_load(2, q).start()
    for q in range(PIECES):
        fwd_y[q].wait_recv()
    for q in range(PIECES):
        nxt_load(3, q).start()

    def layer1(src, finish):
        values = x1[src].astype(F32)
        hid[0] = (normalize(values) * row(ln, 1)).astype(BF16)
        if finish:
            acc[0] = values + row(bo, 1) + row(b2, 1)
        else:
            acc[0] = jnp.zeros((seq, dim), F32)

        @pl.loop(0, 4)
        def _(slot):
            acc[0] += attend(0, slot, 1) + mlp_part(0, slot, 1, 0, mlp)

    def rows_of(chip_x, chip_y, core, k):
        return pl.ds(((2 * (1 - chip_x) + core) * IMGS + OWN * chip_y + k) * seq, seq)

    def put(k):
        rows = rows_of(x, y, c, k)
        return (
            pltpu.make_async_copy(fin.at[k], out.at[rows, :], s_out.at[k]),
            remote(fin.at[k], out.at[rows, :], s_oc.at[k], r_oc.at[k], cp),
            remote(fin.at[k], out.at[rows, :], s_ox.at[k], r_ox.at[k], xp),
            remote(fin.at[k], out.at[rows, :], s_oy.at[k], r_oy.at[k], yp),
        )

    def pass_on(k):
        of_x = out.at[rows_of(1 - x, y, c, k), :]
        of_y = out.at[rows_of(x, 1 - y, c, k), :]
        of_d = out.at[rows_of(1 - x, 1 - y, c, k), :]
        return (
            remote(of_x, of_x, s_od.at[k], r_od.at[k], yp),
            remote(of_x, of_x, s_ex.at[k], r_ex.at[k], cp),
            remote(of_y, of_y, s_ey.at[k], r_ey.at[k], cp),
            remote(of_d, of_d, s_ed.at[k], r_ed.at[k], cp),
        )

    def come(k):
        of_c = out.at[rows_of(x, y, 1 - c, k), :]
        of_x = out.at[rows_of(1 - x, y, c, k), :]
        of_y = out.at[rows_of(x, 1 - y, c, k), :]
        of_d = out.at[rows_of(1 - x, 1 - y, c, k), :]
        of_cx = out.at[rows_of(1 - x, y, 1 - c, k), :]
        of_cy = out.at[rows_of(x, 1 - y, 1 - c, k), :]
        of_cd = out.at[rows_of(1 - x, 1 - y, 1 - c, k), :]
        return (
            remote(of_c, of_c, s_oc.at[k], r_oc.at[k], cp),
            remote(of_x, of_x, s_ox.at[k], r_ox.at[k], xp),
            remote(of_y, of_y, s_oy.at[k], r_oy.at[k], yp),
            remote(of_d, of_d, s_od.at[k], r_od.at[k], yp),
            remote(of_cx, of_cx, s_ex.at[k], r_ex.at[k], cp),
            remote(of_cy, of_cy, s_ey.at[k], r_ey.at[k], cp),
            remote(of_cd, of_cd, s_ed.at[k], r_ed.at[k], cp),
        )

    def near(k):
        part0(k).wait_recv()
        x1[k] = (acc[OWN + k] + rcv0[k].astype(F32)).astype(BF16)
        give0(k).start()

    def near_layer1(k):
        layer1(k, False)
        snd1[k] = acc[0].astype(BF16)
        part1(k).start()

    def far(k):
        give0(k).wait_recv()
        layer1(OWN + k, True)
        part1(k).wait_recv()
        fin[k] = (acc[0] + rcv1[k].astype(F32)).astype(BF16)
        for copy in put(k):
            copy.start()

    @pl.loop(0, OWN)
    def _(k):
        near(k)

        @pl.when(k == 0)
        def _():
            for slot in range(4):
                for q in range(PIECES):
                    nxt_load(slot, q).wait()

        near_layer1(k)

        @pl.when(k >= 1)
        def _():
            far(k - 1)

    far(OWN - 1)

    @pl.loop(0, OWN)
    def _(k):
        to_d, to_cx, to_cy, _ = pass_on(k)
        _, by_x, by_y, _, _, _, _ = come(k)
        by_y.wait_recv()
        to_cy.start()
        by_x.wait_recv()
        to_d.start()
        to_cx.start()

    @pl.loop(0, OWN)
    def _(k):
        come(k)[3].wait_recv()
        pass_on(k)[3].start()

    @pl.loop(0, OWN)
    def _(k):
        by_c, _, _, _, by_cx, by_cy, by_cd = come(k)
        for copy in (by_c, by_cx, by_cy, by_cd):
            copy.wait_recv()
        local, *others = put(k)
        local.wait()
        for copy in (*others, *pass_on(k), part0(k), give0(k), part1(k)):
            copy.wait_send()

    for copy in biases:
        copy.wait_send()
    for q in range(PIECES):
        own_core[q].wait_send()
        own_x[q].wait_send()
        nxt_core[q].wait_send()
        nxt_y[q].wait_send()
        fwd_y[q].wait_send()


def solution(mesh):
    col_spec = P(None, None, "tp")
    row_spec = P(None, "tp", None)
    in_specs = (P("dp", None, None), P(), col_spec, col_spec, col_spec, P(), P(), row_spec, P(), col_spec, P(None, "tp"), row_spec, P())

    def per_device(tokens_in, ln_scale, w_query, w_key, w_value, q_scale, k_scale, w_out, b_out, w_up, b_up, w_down, b_down):
        n_images, seq, dim = tokens_in.shape
        layers, _, heads_w = w_query.shape
        mlp = w_up.shape[2]
        across = lambda w: jnp.swapaxes(w, 1, 2)
        any_spec = pl.BlockSpec(memory_space=pl.ANY)
        vm_spec = pl.BlockSpec(memory_space=pltpu.VMEM)
        dma = lambda *shape: pltpu.SemaphoreType.DMA(shape)
        shape = jax.ShapeDtypeStruct
        encoded, *_ = pl.pallas_call(
            fused,
            out_shape=(
                shape((n_images * seq, dim), BF16),
                shape((3, 3 * heads_w, dim), BF16),
                shape((3, heads_w, dim), BF16),
                shape((3, dim, mlp), BF16),
                shape((3, mlp, dim), BF16),
            ),
            in_specs=[any_spec] * 7 + [vm_spec] * 6,
            out_specs=(any_spec,) * 5,
            scratch_shapes=[
                pltpu.VMEM((4, 3 * heads_w, dim), BF16),
                pltpu.VMEM((4, heads_w, dim), BF16),
                pltpu.VMEM((4, dim, mlp), BF16),
                pltpu.VMEM((4, mlp, dim), BF16),
                pltpu.VMEM((6, layers, mlp), BF16),
                pltpu.VMEM((layers, 2, q_scale.shape[1], seq), F32),
                pltpu.VMEM((IMGS, seq, dim), F32),
                pltpu.VMEM((IMGS, seq, dim), BF16),
                pltpu.VMEM((IMGS, seq, dim), BF16),
                *[pltpu.VMEM((OWN, seq, dim), BF16)] * 5,
                dma(PIECES), dma(4, PIECES), dma(IMGS), dma(5), dma(5),
                *[dma(PIECES)] * 12,
                *[dma(OWN)] * 6,
                *[dma(OWN)] * 9,
                *[dma(OWN)] * 6,
            ],
            compiler_params=pltpu.CompilerParams(
                collective_id=0, has_side_effects=True, vmem_limit_bytes=67000000),
        )(tokens_in.reshape(n_images * seq, dim), across(w_query), across(w_key), across(w_value), w_out, w_up, w_down, ln_scale, q_scale, k_scale, b_out, b_up, b_down)
        return encoded.reshape(n_images, seq, dim)

    return jax.shard_map(per_device, mesh=mesh, in_specs=in_specs, out_specs=P("dp", None, None), check_vma=False)
```

```python
import jax
import jax.numpy as jnp
from jax import lax
from jax.experimental import pallas as pl
from jax.experimental.pallas import tpu as pltpu
from jax.sharding import PartitionSpec as P

LN_EPS = 1e-6
MESH = pl.DeviceIdType.MESH
F32, BF16 = jnp.float32, jnp.bfloat16

IMGS = 8
OWN = 4
SPLIT = 384
PIECES = 8
CUTS = 4
HALVES = 2


def normalize(values):
    mean_val = jnp.mean(values, axis=-1, keepdims=True)
    centered = values - mean_val
    variance = jnp.mean(centered * centered, axis=-1, keepdims=True)
    return centered * lax.rsqrt(variance + LN_EPS)


def gelu(pre):
    inner = (2.0 / jnp.pi) ** 0.5 * (pre + 0.044715 * (pre * pre * pre))
    return pre * (0.5 * (1.0 + jnp.tanh(inner)))


def dot(lhs, rhs):
    return jnp.dot(lhs, rhs, preferred_element_type=F32)


def fused(
    tok, wq, wk, wv, wo, w1, w2, ln, qs, ks, bo, bu, b2,
    out, gq, go, g1, g2,
    vq, vo, v1, v2, vb, gain, acc, hid, x1, snd0, rcv0, snd1, rcv1, fin,
    loc0, loc1, xs, s_b, r_b,
    s_c0, r_c0, s_x0, r_x0, s_f0, r_f0,
    s_c1, r_c1, s_y1, r_y1, s_f1, r_f1,
    s_p0, r_p0, s_g0, r_g0, s_p1, r_p1,
    s_out, s_oc, r_oc, s_ox, r_ox, s_oy, r_oy, s_od, r_od,
    s_ex, r_ex, s_ey, r_ey, s_ed, r_ed,
):
    seq, dim = hid.shape[1], hid.shape[2]
    heads_w = wo.shape[1]
    head_dim = qs.shape[1]
    n_heads = heads_w // head_dim
    mlp = w1.shape[2]
    me = lax.axis_index("tp")
    y = me // 4
    x = (me // 2) % 2
    c = me % 2
    cp = me + 1 - 2 * c
    xp = me + 2 - 4 * x
    yp = me + 4 - 8 * y
    xc = xp + 1 - 2 * c
    yc = yp + 1 - 2 * c

    def remote(src, dst, send, recv, dev):
        return pltpu.make_async_remote_copy(
            src_ref=src, dst_ref=dst, send_sem=send, recv_sem=recv,
            device_id={"tp": dev}, device_id_type=MESH)

    def pieces_of(layer):
        return (
            wq.at[layer], wk.at[layer], wv.at[layer], wo.at[layer],
            w1.at[layer, :, pl.ds(0, SPLIT)], w2.at[layer, pl.ds(0, SPLIT), :],
            w1.at[layer, :, pl.ds(SPLIT, mlp - SPLIT)], w2.at[layer, pl.ds(SPLIT, mlp - SPLIT), :],
        )

    def slot_of(refs, slot):
        a, b, d, e = refs
        third = [a.at[slot, pl.ds(n * heads_w, heads_w), :] for n in range(3)]
        return (
            *third, b.at[slot],
            d.at[slot, :, pl.ds(0, SPLIT)], e.at[slot, pl.ds(0, SPLIT), :],
            d.at[slot, :, pl.ds(SPLIT, mlp - SPLIT)], e.at[slot, pl.ds(SPLIT, mlp - SPLIT), :],
        )

    vmem = (vq, vo, v1, v2)
    land = (gq, go, g1, g2)

    def moves(src, dst, send, recv, dev):
        return [remote(src[q], dst[q], send.at[q], recv.at[q], dev) for q in range(PIECES)]

    own_load = [pltpu.make_async_copy(pieces_of(0)[q], slot_of(vmem, 0)[q], loc0.at[q]) for q in range(PIECES)]
    own_core = moves(pieces_of(0), slot_of(vmem, 1), s_c0, r_c0, cp)
    own_x = moves(pieces_of(0), slot_of(vmem, 2), s_x0, r_x0, xp)
    fwd_x = moves(slot_of(vmem, 2), slot_of(vmem, 3), s_f0, r_f0, cp)
    nxt_core = moves(pieces_of(1), slot_of(land, 0), s_c1, r_c1, cp)
    nxt_y = moves(pieces_of(1), slot_of(land, 1), s_y1, r_y1, yp)
    fwd_y = moves(slot_of(land, 1), slot_of(land, 2), s_f1, r_f1, cp)
    peers = (cp, xp, xc, yp, yc)
    biases = [remote(bu, vb.at[n + 1], s_b.at[n], r_b.at[n], peers[n]) for n in range(5)]

    def nxt_load(slot, q):
        src = pieces_of(1) if slot == 0 else slot_of(land, slot - 1)
        return pltpu.make_async_copy(src[q], slot_of(vmem, slot)[q], loc1.at[slot, q])

    group = (2 * x + c) * IMGS

    def image_of(i):
        far = (i < OWN).astype(jnp.int32) if not isinstance(i, int) else int(i < OWN)
        return group + OWN * (y + far - 2 * y * far) + i % OWN

    def load_x(i):
        return pltpu.make_async_copy(tok.at[pl.ds(image_of(i) * seq, seq), :], hid.at[i], xs.at[i])

    barrier = pltpu.get_barrier_semaphore()
    for dev in peers:
        pl.semaphore_signal(barrier, inc=1, device_id={"tp": dev}, device_id_type=MESH)
    for q in range(PIECES):
        own_load[q].start()
    for i in range(IMGS):
        load_x(i).start()
    pl.semaphore_wait(barrier, len(peers))

    for copy in biases:
        copy.start()
    for q in range(PIECES):
        own_x[q].start()
        nxt_y[q].start()
        own_core[q].start()
    for q in range(PIECES):
        nxt_core[q].start()

    def row(ref, layer):
        return ref[layer : layer + 1, :].astype(F32)

    vb[0] = bu[...]
    for layer in range(2):
        for n, ref in enumerate((qs, ks)):
            gain[layer, n] = jnp.broadcast_to(row(ref, layer), (seq, head_dim)).T

    def head_norm(values, layer, n):
        mean_val = jnp.mean(values, axis=0, keepdims=True)
        centered = values - mean_val
        variance = jnp.mean(centered * centered, axis=0, keepdims=True)
        return centered * lax.rsqrt(variance + LN_EPS) * gain[layer, n]

    def attend(i, slot, layer):
        proj = lax.dot_general(vq[slot], hid[i], (((1,), (1,)), ((), ())), preferred_element_type=F32)
        mixed = []
        for hd in range(n_heads):
            lo = hd * head_dim
            q_h = head_norm(proj[lo : lo + head_dim], layer, 0).astype(BF16)
            k_h = head_norm(proj[heads_w + lo : heads_w + lo + head_dim], layer, 1).T.astype(BF16)
            v_h = proj[2 * heads_w + lo : 2 * heads_w + lo + head_dim].astype(BF16)
            scores = dot(k_h, q_h) * head_dim ** -0.5
            weight = jnp.exp(scores - jnp.max(scores, axis=0, keepdims=True))
            total = jnp.sum(weight, axis=0, keepdims=True)
            prob = (weight * (1.0 / total)).astype(BF16)
            mixed.append(dot(v_h, prob))
        mix = jnp.concatenate(mixed, axis=0).T.astype(BF16)
        return dot(mix, vo[slot])

    def mlp_part(i, slot, layer, lo, hi):
        bias = vb[slot + 2 * layer * (slot // 2), layer : layer + 1, lo:hi].astype(F32)
        act = gelu(dot(hid[i], v1[slot, :, lo:hi]) + bias).astype(BF16)
        return dot(act, v2[slot, lo:hi, :])

    @pl.loop(0, IMGS)
    def _(i):
        load_x(i).wait()
        values = hid[i].astype(F32)
        hid[i] = (normalize(values) * row(ln, 0)).astype(BF16)

        @pl.when(i < OWN)
        def _():
            acc[i] = jnp.zeros((seq, dim), F32)

        @pl.when(i >= OWN)
        def _():
            acc[i] = values + row(bo, 0) + row(b2, 0)

    @pl.loop(0, 2)
    def _(slot):
        @pl.when(slot == 0)
        def _():
            for q in range(PIECES):
                own_load[q].wait()
            for copy in biases:
                copy.wait_recv()

        @pl.when(slot == 1)
        def _():
            for q in range(PIECES):
                own_core[q].wait_recv()

        @pl.loop(0, IMGS)
        def _(i):
            acc[i] += attend(i, slot, 0) + mlp_part(i, slot, 0, 0, mlp)

    for q in range(PIECES):
        nxt_core[q].wait_recv()
    for q in range(PIECES):
        nxt_load(0, q).start()
        nxt_load(1, q).start()

    def arrive(slot, pieces):
        @pl.when(slot == 2)
        def _():
            for q in pieces:
                own_x[q].wait_recv()
                fwd_x[q].start()

        @pl.when(slot == 3)
        def _():
            for q in pieces:
                fwd_x[q].wait_recv()

    @pl.loop(2, 4)
    def _(slot):
        arrive(slot, (0, 1, 2, 3))

        @pl.loop(0, IMGS)
        def _(i):
            acc[i] += attend(i, slot, 0)

    for q in range(4):
        nxt_y[q].wait_recv()
        fwd_y[q].start()

    @pl.loop(2, 4)
    def _(slot):
        arrive(slot, (4, 5))

        @pl.loop(0, IMGS)
        def _(i):
            acc[i] += mlp_part(i, slot, 0, 0, SPLIT)

    for q in (4, 5):
        nxt_y[q].wait_recv()
        fwd_y[q].start()

    for q in (6, 7):
        own_x[q].wait_recv()
        fwd_x[q].start()
    for q in (6, 7):
        fwd_x[q].wait_recv()

    def cut(n):
        return pl.ds(n * (seq // CUTS), seq // CUTS)

    def part0(k, n):
        return remote(snd0.at[k, cut(n), :], rcv0.at[k, cut(n), :], s_p0.at[k, n], r_p0.at[k, n], yp)

    def give0(k, n):
        return remote(x1.at[k, cut(n), :], x1.at[OWN + k, cut(n), :], s_g0.at[k, n], r_g0.at[k, n], xp)

    def part1(k):
        return remote(snd1.at[k], rcv1.at[k], s_p1.at[k], r_p1.at[k], xp)

    @pl.loop(0, IMGS)
    def _(i):
        acc[i] += mlp_part(i, 2, 0, SPLIT, mlp) + mlp_part(i, 3, 0, SPLIT, mlp)

        @pl.when(i < OWN)
        def _():
            snd0[i] = acc[i].astype(BF16)
            for n in range(CUTS):
                part0(i, n).start()

    for q in (6, 7):
        nxt_y[q].wait_recv()
        fwd_y[q].start()
    for q in range(PIECES):
        fwd_x[q].wait_send()
    for q in range(PIECES):
        nxt_load(2, q).start()
    for q in range(PIECES):
        fwd_y[q].wait_recv()
    for q in range(PIECES):
        nxt_load(3, q).start()

    def layer1(src, finish):
        values = x1[src].astype(F32)
        hid[0] = (normalize(values) * row(ln, 1)).astype(BF16)
        if finish:
            acc[0] = values + row(bo, 1) + row(b2, 1)
        else:
            acc[0] = jnp.zeros((seq, dim), F32)

        @pl.loop(0, 4)
        def _(slot):
            acc[0] += attend(0, slot, 1) + mlp_part(0, slot, 1, 0, mlp)

    def half_of(chip_x, chip_y, core, k, n):
        image = (2 * (1 - chip_x) + core) * IMGS + OWN * chip_y + k
        return out.at[pl.ds(image * seq + n * (seq // HALVES), seq // HALVES), :]

    def put(k, n):
        src = fin.at[k, pl.ds(n * (seq // HALVES), seq // HALVES), :]
        dst = half_of(x, y, c, k, n)
        return (
            pltpu.make_async_copy(src, dst, s_out.at[k, n]),
            remote(src, dst, s_oc.at[k, n], r_oc.at[k, n], cp),
            remote(src, dst, s_oy.at[k, n], r_oy.at[k, n], yp),
            remote(src, dst, s_ox.at[k, n], r_ox.at[k, n], xp),
        )

    def pass_on(k, n):
        of_x = half_of(1 - x, y, c, k, n)
        of_y = half_of(x, 1 - y, c, k, n)
        of_d = half_of(1 - x, 1 - y, c, k, n)
        return (
            remote(of_x, of_x, s_od.at[k, n], r_od.at[k, n], yp),
            remote(of_x, of_x, s_ex.at[k, n], r_ex.at[k, n], cp),
            remote(of_y, of_y, s_ey.at[k, n], r_ey.at[k, n], cp),
            remote(of_d, of_d, s_ed.at[k, n], r_ed.at[k, n], cp),
        )

    def come(k, n):
        def into(ref, recv):
            return remote(ref, ref, s_out.at[k, n], recv.at[k, n], cp)

        return (
            into(half_of(1 - x, y, c, k, n), r_ox),
            into(half_of(x, 1 - y, c, k, n), r_oy),
            into(half_of(1 - x, 1 - y, c, k, n), r_od),
            into(half_of(x, y, 1 - c, k, n), r_oc),
            into(half_of(1 - x, y, 1 - c, k, n), r_ex),
            into(half_of(x, 1 - y, 1 - c, k, n), r_ey),
            into(half_of(1 - x, 1 - y, 1 - c, k, n), r_ed),
        )

    def near(k):
        for n in range(CUTS):
            part0(k, n).wait_recv()
            x1[k, cut(n), :] = (acc[OWN + k, cut(n), :] + rcv0[k, cut(n), :].astype(F32)).astype(BF16)
            give0(k, n).start()

    def near_layer1(k):
        layer1(k, False)
        snd1[k] = acc[0].astype(BF16)
        part1(k).start()

    def far(k):
        for n in range(CUTS):
            give0(k, n).wait_recv()
        layer1(OWN + k, True)
        part1(k).wait_recv()
        fin[k] = (acc[0] + rcv1[k].astype(F32)).astype(BF16)
        for n in range(HALVES):
            for copy in put(k, n)[:3]:
                copy.start()

    def far_x(k):
        for n in range(HALVES):
            put(k, n)[3].start()

    near(0)
    for slot in range(4):
        for q in range(PIECES):
            nxt_load(slot, q).wait()

    @pl.loop(0, OWN)
    def _(k):
        near_layer1(k)

        @pl.when(k < OWN - 1)
        def _():
            near(k + 1)

        @pl.when(k == OWN - 1)
        def _():
            for early in range(OWN - 2):
                far_x(early)

        @pl.when(k >= 1)
        def _():
            far(k - 1)

    far_x(OWN - 2)
    far(OWN - 1)
    far_x(OWN - 1)

    lag = 2

    @pl.loop(0, OWN * HALVES + lag)
    def _(j):
        @pl.when(j < OWN * HALVES)
        def _():
            k, n = j // HALVES, j % HALVES
            by_x, by_y, *_ = come(k, n)
            to_d, x_core, y_core, _ = pass_on(k, n)
            by_y.wait_recv()
            y_core.start()
            by_x.wait_recv()
            to_d.start()
            x_core.start()

        @pl.when(j >= lag)
        def _():
            k, n = (j - lag) // HALVES, (j - lag) % HALVES
            come(k, n)[2].wait_recv()
            pass_on(k, n)[3].start()

    @pl.loop(0, OWN)
    def _(k):
        part1(k).wait_send()
        for n in range(CUTS):
            part0(k, n).wait_send()
            give0(k, n).wait_send()
        for n in range(HALVES):
            local, *others = put(k, n)
            local.wait()
            for copy in (*others, *pass_on(k, n)):
                copy.wait_send()
            for copy in come(k, n)[3:]:
                copy.wait_recv()

    for copy in biases:
        copy.wait_send()
    for q in range(PIECES):
        own_core[q].wait_send()
        own_x[q].wait_send()
        nxt_core[q].wait_send()
        nxt_y[q].wait_send()
        fwd_y[q].wait_send()


def solution(mesh):
    col_spec = P(None, None, "tp")
    row_spec = P(None, "tp", None)
    in_specs = (P("dp", None, None), P(), col_spec, col_spec, col_spec, P(), P(), row_spec, P(), col_spec, P(None, "tp"), row_spec, P())

    def per_device(tokens_in, ln_scale, w_query, w_key, w_value, q_scale, k_scale, w_out, b_out, w_up, b_up, w_down, b_down):
        n_images, seq, dim = tokens_in.shape
        layers, _, heads_w = w_query.shape
        mlp = w_up.shape[2]
        across = lambda w: jnp.swapaxes(w, 1, 2)
        any_spec = pl.BlockSpec(memory_space=pl.ANY)
        vm_spec = pl.BlockSpec(memory_space=pltpu.VMEM)
        dma = lambda *shape: pltpu.SemaphoreType.DMA(shape)
        shape = jax.ShapeDtypeStruct
        encoded, *_ = pl.pallas_call(
            fused,
            out_shape=(
                shape((n_images * seq, dim), BF16),
                shape((3, 3 * heads_w, dim), BF16),
                shape((3, heads_w, dim), BF16),
                shape((3, dim, mlp), BF16),
                shape((3, mlp, dim), BF16),
            ),
            in_specs=[any_spec] * 7 + [vm_spec] * 6,
            out_specs=(any_spec,) * 5,
            scratch_shapes=[
                pltpu.VMEM((4, 3 * heads_w, dim), BF16),
                pltpu.VMEM((4, heads_w, dim), BF16),
                pltpu.VMEM((4, dim, mlp), BF16),
                pltpu.VMEM((4, mlp, dim), BF16),
                pltpu.VMEM((6, layers, mlp), BF16),
                pltpu.VMEM((layers, 2, q_scale.shape[1], seq), F32),
                pltpu.VMEM((IMGS, seq, dim), F32),
                pltpu.VMEM((IMGS, seq, dim), BF16),
                pltpu.VMEM((IMGS, seq, dim), BF16),
                *[pltpu.VMEM((OWN, seq, dim), BF16)] * 5,
                dma(PIECES), dma(4, PIECES), dma(IMGS), dma(5), dma(5),
                *[dma(PIECES)] * 12,
                *[dma(OWN, CUTS)] * 4, dma(OWN), dma(OWN),
                *[dma(OWN, HALVES)] * 15,
            ],
            compiler_params=pltpu.CompilerParams(
                collective_id=0, has_side_effects=True, vmem_limit_bytes=67000000),
        )(tokens_in.reshape(n_images * seq, dim), across(w_query), across(w_key), across(w_value), w_out, w_up, w_down, ln_scale, q_scale, k_scale, b_out, b_up, b_down)
        return encoded.reshape(n_images, seq, dim)

    return jax.shard_map(per_device, mesh=mesh, in_specs=in_specs, out_specs=P("dp", None, None), check_vma=False)
```

```python
import jax
import jax.numpy as jnp
from jax import lax
from jax.experimental import pallas as pl
from jax.experimental.pallas import tpu as pltpu
from jax.sharding import PartitionSpec as P

LN_EPS = 1e-6
MESH = pl.DeviceIdType.MESH
F32, BF16 = jnp.float32, jnp.bfloat16

IMGS = 8
OWN = 4
SPLIT = 384
PIECES = 8
CUTS = 4
PARTS = 4
TURN = 14


def normalize(values):
    mean_val = jnp.mean(values, axis=-1, keepdims=True)
    centered = values - mean_val
    variance = jnp.mean(centered * centered, axis=-1, keepdims=True)
    return centered * lax.rsqrt(variance + LN_EPS)


def gelu(pre):
    inner = (2.0 / jnp.pi) ** 0.5 * (pre + 0.044715 * (pre * pre * pre))
    return pre * (0.5 * (1.0 + jnp.tanh(inner)))


def dot(lhs, rhs):
    return jnp.dot(lhs, rhs, preferred_element_type=F32)


def fused(
    tok, wq, wk, wv, wo, w1, w2, ln, qs, ks, bo, bu, b2,
    out, gq, go, g1, g2,
    vq, vo, v1, v2, vb, gain, acc, hid, x1,
    loc0, loc1, xs, s_b, r_b,
    s_c0, r_c0, s_x0, r_x0, s_f0, r_f0,
    s_c1, r_c1, s_y1, r_y1, s_f1, r_f1,
    s_p0, r_p0, s_g0, r_g0, s_p1, r_p1,
    s_oc, r_oc, s_ey, r_ey,
    s_ox, r_ox, s_oy, r_oy, s_od, r_od, s_ex, r_ex, s_ed, r_ed,
):
    seq, dim = hid.shape[1], hid.shape[2]
    heads_w = wo.shape[1]
    head_dim = qs.shape[1]
    n_heads = heads_w // head_dim
    mlp = w1.shape[2]
    me = lax.axis_index("tp")
    y = me // 4
    x = (me // 2) % 2
    c = me % 2
    cp = me + 1 - 2 * c
    xp = me + 2 - 4 * x
    yp = me + 4 - 8 * y
    xc = xp + 1 - 2 * c
    yc = yp + 1 - 2 * c

    def remote(src, dst, send, recv, dev):
        return pltpu.make_async_remote_copy(
            src_ref=src, dst_ref=dst, send_sem=send, recv_sem=recv,
            device_id={"tp": dev}, device_id_type=MESH)

    def pieces_of(layer):
        return (
            wq.at[layer], wk.at[layer], wv.at[layer], wo.at[layer],
            w1.at[layer, :, pl.ds(0, SPLIT)], w2.at[layer, pl.ds(0, SPLIT), :],
            w1.at[layer, :, pl.ds(SPLIT, mlp - SPLIT)], w2.at[layer, pl.ds(SPLIT, mlp - SPLIT), :],
        )

    def slot_of(refs, slot):
        a, b, d, e = refs
        third = [a.at[slot, pl.ds(n * heads_w, heads_w), :] for n in range(3)]
        return (
            *third, b.at[slot],
            d.at[slot, :, pl.ds(0, SPLIT)], e.at[slot, pl.ds(0, SPLIT), :],
            d.at[slot, :, pl.ds(SPLIT, mlp - SPLIT)], e.at[slot, pl.ds(SPLIT, mlp - SPLIT), :],
        )

    vmem = (vq, vo, v1, v2)
    land = (gq, go, g1, g2)

    def moves(src, dst, send, recv, dev):
        return [remote(src[q], dst[q], send.at[q], recv.at[q], dev) for q in range(PIECES)]

    own_load = [pltpu.make_async_copy(pieces_of(0)[q], slot_of(vmem, 0)[q], loc0.at[q]) for q in range(PIECES)]
    own_core = moves(pieces_of(0), slot_of(vmem, 1), s_c0, r_c0, cp)
    own_x = moves(pieces_of(0), slot_of(vmem, 2), s_x0, r_x0, xp)
    fwd_x = moves(slot_of(vmem, 2), slot_of(vmem, 3), s_f0, r_f0, cp)
    nxt_core = moves(pieces_of(1), slot_of(land, 0), s_c1, r_c1, cp)
    nxt_y = moves(pieces_of(1), slot_of(land, 1), s_y1, r_y1, yp)
    fwd_y = moves(slot_of(land, 1), slot_of(land, 2), s_f1, r_f1, cp)
    peers = (cp, xp, xc, yp, yc)
    biases = [remote(bu, vb.at[n + 1], s_b.at[n], r_b.at[n], peers[n]) for n in range(5)]

    def nxt_load(slot, q):
        src = pieces_of(1) if slot == 0 else slot_of(land, slot - 1)
        return pltpu.make_async_copy(src[q], slot_of(vmem, slot)[q], loc1.at[slot, q])

    group = (2 * x + c) * IMGS

    def image_of(i):
        far = (i < OWN).astype(jnp.int32) if not isinstance(i, int) else int(i < OWN)
        return group + OWN * (y + far - 2 * y * far) + i % OWN

    def load_x(i):
        return pltpu.make_async_copy(tok.at[pl.ds(image_of(i) * seq, seq), :], hid.at[i], xs.at[i])

    barrier = pltpu.get_barrier_semaphore()
    for dev in peers:
        pl.semaphore_signal(barrier, inc=1, device_id={"tp": dev}, device_id_type=MESH)
    for q in range(PIECES):
        own_load[q].start()
    for i in range(IMGS):
        load_x(i).start()
    pl.semaphore_wait(barrier, len(peers))

    for copy in biases:
        copy.start()
    for q in range(PIECES):
        own_x[q].start()
        nxt_y[q].start()
        own_core[q].start()
    for q in range(PIECES):
        nxt_core[q].start()

    def row(ref, layer):
        return ref[layer : layer + 1, :].astype(F32)

    vb[0] = bu[...]
    for layer in range(2):
        for n, ref in enumerate((qs, ks)):
            gain[layer, n] = jnp.broadcast_to(row(ref, layer), (seq, head_dim)).T

    def head_norm(values, layer, n):
        mean_val = jnp.mean(values, axis=0, keepdims=True)
        centered = values - mean_val
        variance = jnp.mean(centered * centered, axis=0, keepdims=True)
        return centered * lax.rsqrt(variance + LN_EPS) * gain[layer, n]

    def attend(i, slot, layer):
        proj = lax.dot_general(vq[slot], hid[i], (((1,), (1,)), ((), ())), preferred_element_type=F32)
        mixed = []
        for hd in range(n_heads):
            lo = hd * head_dim
            q_h = head_norm(proj[lo : lo + head_dim], layer, 0).astype(BF16)
            k_h = head_norm(proj[heads_w + lo : heads_w + lo + head_dim], layer, 1).T.astype(BF16)
            v_h = proj[2 * heads_w + lo : 2 * heads_w + lo + head_dim].astype(BF16)
            scores = dot(k_h, q_h) * head_dim ** -0.5
            weight = jnp.exp(scores - jnp.max(scores, axis=0, keepdims=True))
            total = jnp.sum(weight, axis=0, keepdims=True)
            prob = (weight * (1.0 / total)).astype(BF16)
            mixed.append(dot(v_h, prob))
        mix = jnp.concatenate(mixed, axis=0).T.astype(BF16)
        return dot(mix, vo[slot])

    def mlp_part(i, slot, layer, lo, hi):
        bias = vb[slot + 2 * layer * (slot // 2), layer : layer + 1, lo:hi].astype(F32)
        act = gelu(dot(hid[i], v1[slot, :, lo:hi]) + bias).astype(BF16)
        return dot(act, v2[slot, lo:hi, :])

    @pl.loop(0, IMGS)
    def _(i):
        load_x(i).wait()
        values = hid[i].astype(F32)
        hid[i] = (normalize(values) * row(ln, 0)).astype(BF16)

        @pl.when(i < OWN)
        def _():
            acc[i] = jnp.zeros((seq, dim), F32)

        @pl.when(i >= OWN)
        def _():
            acc[i] = values + row(bo, 0) + row(b2, 0)

    @pl.loop(0, 2)
    def _(slot):
        @pl.when(slot == 0)
        def _():
            for q in range(PIECES):
                own_load[q].wait()
            for copy in biases:
                copy.wait_recv()

        @pl.when(slot == 1)
        def _():
            for q in range(PIECES):
                own_core[q].wait_recv()

        @pl.loop(0, IMGS)
        def _(i):
            acc[i] += attend(i, slot, 0) + mlp_part(i, slot, 0, 0, mlp)

    for q in range(PIECES):
        nxt_core[q].wait_recv()
    for q in range(PIECES):
        nxt_load(0, q).start()
        nxt_load(1, q).start()

    def arrive(slot, pieces):
        @pl.when(slot == 2)
        def _():
            for q in pieces:
                own_x[q].wait_recv()
                fwd_x[q].start()

        @pl.when(slot == 3)
        def _():
            for q in pieces:
                fwd_x[q].wait_recv()

    @pl.loop(2, 4)
    def _(slot):
        arrive(slot, (0, 1, 2, 3))

        @pl.loop(0, IMGS)
        def _(i):
            acc[i] += attend(i, slot, 0)

    for q in range(4):
        nxt_y[q].wait_recv()
        fwd_y[q].start()

    @pl.loop(2, 4)
    def _(slot):
        arrive(slot, (4, 5))

        @pl.loop(0, IMGS)
        def _(i):
            acc[i] += mlp_part(i, slot, 0, 0, SPLIT)

    for q in (4, 5):
        nxt_y[q].wait_recv()
        fwd_y[q].start()

    for q in (6, 7):
        own_x[q].wait_recv()
        fwd_x[q].start()
    for q in (6, 7):
        fwd_x[q].wait_recv()

    def cut(n):
        return pl.ds(n * (seq // CUTS), seq // CUTS)

    def rows_of(chip_x, chip_y, core, k):
        return ((2 * (1 - chip_x) + core) * IMGS + OWN * chip_y + k) * seq

    def lent(chip_y, k, n):
        return pl.ds(pl.multiple_of(rows_of(1 - x, chip_y, c, k) + n * (seq // CUTS), seq // CUTS), seq // CUTS)

    def part0(k, n, chip_y):
        return remote(hid.at[k, cut(n), :], out.at[lent(chip_y, k, n), :], s_p0.at[k, n], r_p0.at[k, n], yp)

    def give0(k, n):
        return remote(out.at[lent(y, k, n), :], x1.at[k, cut(n), :], s_g0.at[k, n], r_g0.at[k, n], xp)

    def part1(k, chip_x):
        return remote(hid.at[OWN + k], out.at[pl.ds(rows_of(chip_x, y, c, k), seq), :], s_p1.at[k], r_p1.at[k], xp)

    @pl.loop(0, IMGS)
    def _(i):
        acc[i] += mlp_part(i, 2, 0, SPLIT, mlp) + mlp_part(i, 3, 0, SPLIT, mlp)

        @pl.when(i < OWN)
        def _():
            hid[i] = acc[i].astype(BF16)
            for n in range(CUTS):
                part0(i, n, 1 - y).start()

    for q in (6, 7):
        nxt_y[q].wait_recv()
        fwd_y[q].start()
    for q in range(PIECES):
        fwd_x[q].wait_send()
    for q in range(PIECES):
        nxt_load(2, q).start()
    for q in range(PIECES):
        fwd_y[q].wait_recv()
    for q in range(PIECES):
        nxt_load(3, q).start()

    def layer1(values, finish, between=None):
        values = values.astype(F32)
        hid[0] = (normalize(values) * row(ln, 1)).astype(BF16)
        if finish:
            acc[0] = values + row(bo, 1) + row(b2, 1)
        else:
            acc[0] = jnp.zeros((seq, dim), F32)

        @pl.loop(0, 4)
        def _(slot):
            acc[0] += attend(0, slot, 1) + mlp_part(0, slot, 1, 0, mlp)
            if between is not None:
                between(slot)

    def part_of(chip_x, chip_y, core, k, n):
        return out.at[pl.ds(rows_of(chip_x, chip_y, core, k) + n * (seq // PARTS), seq // PARTS), :]

    def image_at(chip_x, chip_y, core, k):
        return out.at[pl.ds(rows_of(chip_x, chip_y, core, k), seq), :]

    def put_core(k):
        ref = image_at(x, y, c, k)
        return remote(ref, ref, s_oc.at[k], r_oc.at[k], cp)

    def pass_y(k):
        ref = image_at(x, 1 - y, c, k)
        return remote(ref, ref, s_ey.at[k], r_ey.at[k], cp)

    def come_core(k):
        own, of_y = image_at(x, y, 1 - c, k), image_at(x, 1 - y, 1 - c, k)
        return (
            remote(own, own, s_oc.at[k], r_oc.at[k], cp),
            remote(of_y, of_y, s_ey.at[k], r_ey.at[k], cp),
        )

    def put(k, n):
        ref = part_of(x, y, c, k, n)
        return (
            remote(ref, ref, s_oy.at[k, n], r_oy.at[k, n], yp),
            remote(ref, ref, s_ox.at[k, n], r_ox.at[k, n], xp),
        )

    def pass_on(k, n):
        of_x = part_of(1 - x, y, c, k, n)
        of_y = part_of(x, 1 - y, c, k, n)
        of_d = part_of(1 - x, 1 - y, c, k, n)
        return (
            remote(of_x, of_x, s_od.at[k, n], r_od.at[k, n], yp),
            remote(of_y, of_y, s_od.at[k, n], r_od.at[k, n], xp),
            remote(of_x, of_x, s_ex.at[k, n], r_ex.at[k, n], cp),
            remote(of_d, of_d, s_ed.at[k, n], r_ed.at[k, n], cp),
        )

    def come(k, n):
        def into(ref, recv):
            return remote(ref, ref, s_ox.at[k, n], recv.at[k, n], cp)

        return (
            into(part_of(1 - x, y, c, k, n), r_ox),
            into(part_of(x, 1 - y, c, k, n), r_oy),
            into(part_of(1 - x, 1 - y, c, k, n), r_od),
            into(part_of(1 - x, y, 1 - c, k, n), r_ex),
            into(part_of(1 - x, 1 - y, 1 - c, k, n), r_ed),
        )

    def near(k, n):
        part0(k, n, y).wait_recv()
        rows = lent(y, k, n)
        out[rows, :] = (acc[OWN + k, cut(n), :] + out[rows, :].astype(F32)).astype(BF16)
        give0(k, n).start()

    def near_behind(k, when):
        def between(slot):
            @pl.when(when & (slot >= 1))
            def _():
                near(k, slot - 1)

        def rest():
            @pl.when(when)
            def _():
                near(k, CUTS - 1)

        return between, rest

    def near_layer1(k):
        between, rest = near_behind(k + 1, k < OWN - 2)
        rows = pl.ds(pl.multiple_of(rows_of(1 - x, y, c, k), seq), seq)
        layer1(out[rows, :], False, between)
        hid[OWN + k] = acc[0].astype(BF16)
        for n in range(CUTS):
            give0(k, n).wait_send()
        part1(k, 1 - x).start()
        rest()

    def far(k, before=None):
        for n in range(CUTS):
            give0(k, n).wait_recv()
        if before is None:
            between, rest = near_behind(OWN - 1, k == 0)
            layer1(x1[k], True, between)
            rest()
        else:
            layer1(x1[k], True)
            before()
        part1(k, x).wait_recv()
        rows = pl.ds(pl.multiple_of(rows_of(x, y, c, k), seq), seq)
        out[rows, :] = (acc[0] + out[rows, :].astype(F32)).astype(BF16)
        put_core(k).start()
        for n in range(PARTS):
            for copy in put(k, n):
                copy.start()

    def pass_x(k, n):
        come(k, n)[0].wait_recv()
        to_d, _, x_core, _ = pass_on(k, n)

        @pl.when(k * PARTS + n < TURN)
        def _():
            to_d.start()

        x_core.start()

    def pass_x_all(k):
        for n in range(PARTS):
            pass_x(k, n)

    for n in range(CUTS):
        near(0, n)
    for n in range(CUTS):
        part0(0, n, 1 - y).wait_send()
    for slot in range(4):
        for q in range(PIECES):
            nxt_load(slot, q).wait()

    @pl.loop(0, OWN)
    def _(k):
        near_layer1(k)

        @pl.when(k == OWN - 1)
        def _():
            pass_x_all(0)

        @pl.when(k >= 1)
        def _():
            far(k - 1)

    far(OWN - 1, lambda: pass_x_all(1))

    for copy in biases:
        copy.wait_send()
    for q in range(PIECES):
        for copies in (own_core, own_x, nxt_core, nxt_y, fwd_y):
            copies[q].wait_send()
    for k in range(OWN):
        part1(k, 1 - x).wait_send()
        for n in range(CUTS):
            if k > 0:
                part0(k, n, 1 - y).wait_send()

    early, lag, last = 2, 6, 8
    total = OWN * PARTS

    @pl.loop(0, total + last)
    def _(j):
        @pl.when(j < total)
        def _():
            k, n = j // PARTS, j % PARTS
            come(k, n)[1].wait_recv()

            @pl.when(j >= TURN)
            def _():
                pass_on(k, n)[1].start()

            @pl.when(n == PARTS - 1)
            def _():
                pass_y(k).start()

        @pl.when((j >= early * PARTS) & (j < total))
        def _():
            pass_x(j // PARTS, j % PARTS)

        @pl.when((j >= lag) & (j < total + lag))
        def _():
            k, n = (j - lag) // PARTS, (j - lag) % PARTS
            come(k, n)[2].wait_recv()
            pass_on(k, n)[3].start()

        @pl.when(j >= last)
        def _():
            k, n = (j - last) // PARTS, (j - last) % PARTS
            for copy in (*put(k, n), *pass_on(k, n)[1:]):
                copy.wait_send()
            for copy in come(k, n)[3:]:
                copy.wait_recv()

            @pl.when(n == PARTS - 1)
            def _():
                for copy in (put_core(k), pass_y(k)):
                    copy.wait_send()
                for copy in come_core(k):
                    copy.wait_recv()


def solution(mesh):
    col_spec = P(None, None, "tp")
    row_spec = P(None, "tp", None)
    in_specs = (P("dp", None, None), P(), col_spec, col_spec, col_spec, P(), P(), row_spec, P(), col_spec, P(None, "tp"), row_spec, P())

    def per_device(tokens_in, ln_scale, w_query, w_key, w_value, q_scale, k_scale, w_out, b_out, w_up, b_up, w_down, b_down):
        n_images, seq, dim = tokens_in.shape
        layers, _, heads_w = w_query.shape
        mlp = w_up.shape[2]
        across = lambda w: jnp.swapaxes(w, 1, 2)
        any_spec = pl.BlockSpec(memory_space=pl.ANY)
        vm_spec = pl.BlockSpec(memory_space=pltpu.VMEM)
        dma = lambda *shape: pltpu.SemaphoreType.DMA(shape)
        shape = jax.ShapeDtypeStruct
        encoded, *_ = pl.pallas_call(
            fused,
            out_shape=(
                pltpu.VMEM((n_images * seq, dim), BF16),
                shape((3, 3 * heads_w, dim), BF16),
                shape((3, heads_w, dim), BF16),
                shape((3, dim, mlp), BF16),
                shape((3, mlp, dim), BF16),
            ),
            in_specs=[any_spec] * 7 + [vm_spec] * 6,
            out_specs=(vm_spec,) + (any_spec,) * 4,
            scratch_shapes=[
                pltpu.VMEM((4, 3 * heads_w, dim), BF16),
                pltpu.VMEM((4, heads_w, dim), BF16),
                pltpu.VMEM((4, dim, mlp), BF16),
                pltpu.VMEM((4, mlp, dim), BF16),
                pltpu.VMEM((6, layers, mlp), BF16),
                pltpu.VMEM((layers, 2, q_scale.shape[1], seq), F32),
                pltpu.VMEM((IMGS, seq, dim), F32),
                pltpu.VMEM((IMGS, seq, dim), BF16),
                pltpu.VMEM((OWN, seq, dim), BF16),
                dma(PIECES), dma(4, PIECES), dma(IMGS), dma(5), dma(5),
                *[dma(PIECES)] * 12,
                *[dma(OWN, CUTS)] * 4, dma(OWN), dma(OWN),
                *[dma(OWN)] * 4,
                *[dma(OWN, PARTS)] * 10,
            ],
            compiler_params=pltpu.CompilerParams(
                collective_id=0, has_side_effects=True, vmem_limit_bytes=45500000),
        )(tokens_in.reshape(n_images * seq, dim), across(w_query), across(w_key), across(w_value), w_out, w_up, w_down, ln_scale, q_scale, k_scale, b_out, b_up, b_down)
        return encoded.reshape(n_images, seq, dim)

    return jax.shard_map(per_device, mesh=mesh, in_specs=in_specs, out_specs=P("dp", None, None), check_vma=False)
```

```python
import jax
import jax.numpy as jnp
from jax import lax
from jax.experimental import pallas as pl
from jax.experimental.pallas import tpu as pltpu
from jax.sharding import PartitionSpec as P

LN_EPS = 1e-6
MESH = pl.DeviceIdType.MESH
F32, BF16 = jnp.float32, jnp.bfloat16

IMGS = 8
OWN = 4
SPLIT = 384
PIECES = 8
CUTS = 4
PARTS = CUTS
TURN = 14


def normalize(values):
    mean_val = jnp.mean(values, axis=-1, keepdims=True)
    centered = values - mean_val
    variance = jnp.mean(centered * centered, axis=-1, keepdims=True)
    return centered * lax.rsqrt(variance + LN_EPS)


def gelu(pre):
    inner = (2.0 / jnp.pi) ** 0.5 * (pre + 0.044715 * (pre * pre * pre))
    return pre * (0.5 * (1.0 + jnp.tanh(inner)))


def dot(lhs, rhs):
    return jnp.dot(lhs, rhs, preferred_element_type=F32)


def fused(
    tok, wq, wk, wv, wo, w1, w2, bu, ln_in, qs_in, ks_in, bo_in, b2_in,
    out, gq, go, g1, g2,
    vq, vo, v1, v2, vb, ln, qs, ks, bo, b2, gain, acc, hid, x1, s_v,
    loc0, loc1, xs, s_b, r_b,
    s_c0, r_c0, s_x0, r_x0, s_f0, r_f0,
    s_c1, r_c1, s_y1, r_y1, s_f1, r_f1,
    s_p0, r_p0, s_g0, r_g0, s_p1, r_p1,
    s_oc, r_oc, s_ey, r_ey,
    s_ox, r_ox, s_oy, r_oy, s_od, r_od, s_ex, r_ex, s_ed, r_ed,
):
    seq, dim = hid.shape[1], hid.shape[2]
    heads_w = wo.shape[1]
    head_dim = qs.shape[1]
    n_heads = heads_w // head_dim
    mlp = w1.shape[2]
    me = lax.axis_index("tp")
    y = me // 4
    x = (me // 2) % 2
    c = me % 2
    cp = me + 1 - 2 * c
    xp = me + 2 - 4 * x
    yp = me + 4 - 8 * y
    xc = xp + 1 - 2 * c
    yc = yp + 1 - 2 * c

    def remote(src, dst, send, recv, dev):
        return pltpu.make_async_remote_copy(
            src_ref=src, dst_ref=dst, send_sem=send, recv_sem=recv,
            device_id={"tp": dev}, device_id_type=MESH)

    def all_of(sem, rows):
        ref = out.at[pl.ds(0, rows), :]
        return pltpu.make_async_copy(ref, ref, sem)

    def filled(sem, rows):
        all_of(sem, rows).wait()

    sent = filled
    BLOCK = 3 * heads_w + heads_w + 2 * mlp

    def pieces_of(layer):
        return (
            wq.at[layer], wk.at[layer], wv.at[layer], wo.at[layer],
            w1.at[layer, :, pl.ds(0, SPLIT)], w2.at[layer, pl.ds(0, SPLIT), :],
            w1.at[layer, :, pl.ds(SPLIT, mlp - SPLIT)], w2.at[layer, pl.ds(SPLIT, mlp - SPLIT), :],
        )

    def slot_of(refs, slot):
        a, b, d, e = refs
        third = [a.at[slot, pl.ds(n * heads_w, heads_w), :] for n in range(3)]
        return (
            *third, b.at[slot],
            d.at[slot, :, pl.ds(0, SPLIT)], e.at[slot, pl.ds(0, SPLIT), :],
            d.at[slot, :, pl.ds(SPLIT, mlp - SPLIT)], e.at[slot, pl.ds(SPLIT, mlp - SPLIT), :],
        )

    vmem = (vq, vo, v1, v2)
    land = (gq, go, g1, g2)

    def moves(src, dst, send, recv, dev):
        return [remote(src[q], dst[q], send, recv.at[q], dev) for q in range(PIECES)]

    own_load = [pltpu.make_async_copy(pieces_of(0)[q], slot_of(vmem, 0)[q], loc0) for q in range(PIECES)]
    own_core = moves(pieces_of(0), slot_of(vmem, 1), s_c0, r_c0, cp)
    own_x = moves(pieces_of(0), slot_of(vmem, 2), s_x0, r_x0, xp)
    fwd_x = moves(slot_of(vmem, 2), slot_of(vmem, 3), s_f0, r_f0, cp)
    nxt_core = moves(pieces_of(1), slot_of(land, 0), s_c1, r_c1, cp)
    nxt_y = moves(pieces_of(1), slot_of(land, 1), s_y1, r_y1, yp)
    fwd_y = moves(slot_of(land, 1), slot_of(land, 2), s_f1, r_f1, cp)
    peers = (cp, xp, xc, yp, yc)
    biases = [remote(bu, vb.at[n + 1], s_b.at[n], r_b.at[n], peers[n]) for n in range(5)]

    def nxt_load(slot, q):
        src = pieces_of(1) if slot == 0 else slot_of(land, slot - 1)
        return pltpu.make_async_copy(src[q], slot_of(vmem, slot)[q], loc1.at[slot])

    group = (2 * x + c) * IMGS

    def image_of(i):
        far = (i < OWN).astype(jnp.int32) if not isinstance(i, int) else int(i < OWN)
        return group + OWN * (y + far - 2 * y * far) + i % OWN

    def load_x(i):
        return pltpu.make_async_copy(tok.at[pl.ds(image_of(i) * seq, seq), :], hid.at[i], xs.at[i])

    barrier = pltpu.get_barrier_semaphore()
    for dev in peers:
        pl.semaphore_signal(barrier, inc=1, device_id={"tp": dev}, device_id_type=MESH)
    small = [
        pltpu.make_async_copy(src, dst, s_v.at[n])
        for n, (src, dst) in enumerate(
            ((ln_in, ln), (qs_in, qs), (ks_in, ks), (bo_in, bo), (b2_in, b2), (bu, vb.at[0])))
    ]
    for copy in small:
        copy.start()
    for i in range(IMGS):
        load_x(i).start()
    for q in range(PIECES):
        own_load[q].start()
    pl.semaphore_wait(barrier, len(peers))

    for copy in biases:
        copy.start()
    for q in range(PIECES):
        own_x[q].start()
        nxt_y[q].start()
        own_core[q].start()
    for q in range(PIECES):
        nxt_core[q].start()

    def row(ref, layer):
        return ref[layer : layer + 1, :].astype(F32)

    for copy in small:
        copy.wait()
    for layer in range(2):
        for n, ref in enumerate((qs, ks)):
            gain[layer, n] = jnp.broadcast_to(row(ref, layer), (seq, head_dim)).T

    def head_norm(values, layer, n):
        mean_val = jnp.mean(values, axis=0, keepdims=True)
        centered = values - mean_val
        variance = jnp.mean(centered * centered, axis=0, keepdims=True)
        return centered * lax.rsqrt(variance + LN_EPS) * gain[layer, n]

    def heads_of(i, slot):
        return lax.dot_general(vq[slot], hid[i], (((1,), (1,)), ((), ())), preferred_element_type=F32)

    def head_inputs(proj, hd, layer):
        lo = hd * head_dim
        q_h = head_norm(proj[lo : lo + head_dim], layer, 0).astype(BF16)
        k_h = head_norm(proj[heads_w + lo : heads_w + lo + head_dim], layer, 1).astype(BF16).T
        v_h = proj[2 * heads_w + lo : 2 * heads_w + lo + head_dim].astype(BF16)
        return q_h, k_h, v_h

    def softmax(scores):
        scores = scores * head_dim ** -0.5
        weight = jnp.exp(scores - jnp.max(scores, axis=0, keepdims=True))
        total = jnp.sum(weight, axis=0, keepdims=True)
        return (weight * (1.0 / total)).astype(BF16)

    def attend(i, slot, layer):
        proj = heads_of(i, slot)
        parts = [head_inputs(proj, hd, layer) for hd in range(n_heads)]
        scores = [dot(k_h, q_h) for q_h, k_h, _ in parts]
        mixed = [dot(v_h, softmax(sc)) for (_, _, v_h), sc in zip(parts, scores)]
        mix = jnp.concatenate(mixed, axis=0).astype(BF16).T
        return dot(mix, vo[slot])

    def mlp_part(i, slot, layer, lo, hi):
        bias = vb[slot + 2 * layer * (slot // 2), layer : layer + 1, lo:hi].astype(F32)
        act = gelu(dot(hid[i], v1[slot, :, lo:hi]) + bias).astype(BF16)
        return dot(act, v2[slot, lo:hi, :])

    def both(i, slot, layer):
        proj = heads_of(i, slot)
        row_b = vb[slot + 2 * layer * (slot // 2), layer : layer + 1, :].astype(F32)
        bounds = (0, 256, 512, 640)

        def up(n):
            lo, hi = bounds[n], bounds[n + 1]
            return dot(hid[i], v1[slot, :, lo:hi]) + row_b[:, lo:hi]

        def down(n, pre):
            return dot(gelu(pre).astype(BF16), v2[slot, bounds[n] : bounds[n + 1], :])

        pre0 = up(0)
        parts = [head_inputs(proj, hd, layer) for hd in range(n_heads)]
        pre1 = up(1)
        scores = [dot(k_h, q_h) for q_h, k_h, _ in parts]
        pre2 = up(2)
        sum0 = down(0, pre0)
        probs = [softmax(sc) for sc in scores]
        sum1 = down(1, pre1)
        mixed = [dot(v_h, prob) for (_, _, v_h), prob in zip(parts, probs)]
        sum2 = down(2, pre2)
        mix = jnp.concatenate(mixed, axis=0).astype(BF16).T
        return sum0 + sum1 + sum2 + dot(mix, vo[slot])

    @pl.loop(0, IMGS)
    def _(i):
        load_x(i).wait()
        values = hid[i].astype(F32)
        hid[i] = (normalize(values) * row(ln, 0)).astype(BF16)

        @pl.when(i < OWN)
        def _():
            acc[i] = jnp.zeros((seq, dim), F32)

        @pl.when(i >= OWN)
        def _():
            acc[i] = values + row(bo, 0) + row(b2, 0)

    @pl.loop(0, 2)
    def _(slot):
        @pl.when(slot == 0)
        def _():
            filled(loc0, BLOCK)
            for copy in biases:
                copy.wait_recv()

        @pl.when(slot == 1)
        def _():
            for q in range(PIECES):
                own_core[q].wait_recv()

        @pl.loop(0, IMGS)
        def _(i):
            acc[i] += both(i, slot, 0)

    for q in range(PIECES):
        nxt_core[q].wait_recv()
    for q in range(PIECES):
        nxt_load(0, q).start()
        nxt_load(1, q).start()

    def arrive(slot, pieces):
        @pl.when(slot == 2)
        def _():
            for q in pieces:
                own_x[q].wait_recv()
                fwd_x[q].start()

        @pl.when(slot == 3)
        def _():
            for q in pieces:
                fwd_x[q].wait_recv()

    @pl.loop(2, 4)
    def _(slot):
        arrive(slot, (0, 1, 2, 3))

        @pl.loop(0, IMGS)
        def _(i):
            acc[i] += attend(i, slot, 0)

    for q in range(4):
        nxt_y[q].wait_recv()
        fwd_y[q].start()

    @pl.loop(2, 4)
    def _(slot):
        arrive(slot, (4, 5))

        @pl.loop(0, IMGS)
        def _(i):
            acc[i] += mlp_part(i, slot, 0, 0, SPLIT)

    for q in (4, 5):
        nxt_y[q].wait_recv()
        fwd_y[q].start()

    for q in (6, 7):
        own_x[q].wait_recv()
        fwd_x[q].start()
    for q in (6, 7):
        fwd_x[q].wait_recv()

    def cut(n):
        return pl.ds(n * (seq // CUTS), seq // CUTS)

    def rows_of(chip_x, chip_y, core, k):
        return ((2 * (1 - chip_x) + core) * IMGS + OWN * chip_y + k) * seq

    def lent(chip_y, k, n):
        return pl.ds(pl.multiple_of(rows_of(1 - x, chip_y, c, k) + n * (seq // CUTS), seq // CUTS), seq // CUTS)

    def part0(k, n, chip_y):
        return remote(hid.at[k, cut(n), :], out.at[lent(chip_y, k, n), :], s_p0.at[k], r_p0.at[k, n], yp)

    def give0(k, n):
        return remote(out.at[lent(y, k, n), :], x1.at[k, cut(n), :], s_g0.at[k], r_g0.at[k, n], xp)

    def part1(k, n, chip_x):
        rows = pl.ds(pl.multiple_of(rows_of(chip_x, y, c, k) + n * (seq // CUTS), seq // CUTS), seq // CUTS)
        return remote(hid.at[OWN + k, cut(n), :], out.at[rows, :], s_p1, r_p1.at[k, n], xp)

    def near(k, n):
        part0(k, n, y).wait_recv()
        rows = lent(y, k, n)
        out[rows, :] = (acc[OWN + k, cut(n), :] + out[rows, :].astype(F32)).astype(BF16)
        give0(k, n).start()

    @pl.loop(0, OWN)
    def _(k):
        @pl.loop(0, 2)
        def _(mine):
            i = k + OWN * mine
            acc[i] += mlp_part(i, 2, 0, SPLIT, mlp) + mlp_part(i, 3, 0, SPLIT, mlp)

            @pl.when(mine == 0)
            def _():
                hid[k] = acc[k].astype(BF16)
                for n in range(CUTS):
                    part0(k, n, 1 - y).start()

        @pl.when(k == 0)
        def _():
            for q in (6, 7):
                nxt_y[q].wait_recv()
                fwd_y[q].start()

        @pl.when(k >= 1)
        def _():
            near(0, k - 1)

    sent(s_f0, BLOCK)
    for q in range(PIECES):
        nxt_load(2, q).start()
    for q in range(PIECES):
        fwd_y[q].wait_recv()
    for q in range(PIECES):
        nxt_load(3, q).start()

    def layer1(values, finish, between=None):
        values = values.astype(F32)
        hid[0] = (normalize(values) * row(ln, 1)).astype(BF16)
        if finish:
            acc[0] = values + row(bo, 1) + row(b2, 1)
        else:
            acc[0] = jnp.zeros((seq, dim), F32)

        @pl.loop(0, 4)
        def _(slot):
            acc[0] += both(0, slot, 1)
            if between is not None:
                between(slot)

    def part_of(chip_x, chip_y, core, k, n):
        return out.at[pl.ds(rows_of(chip_x, chip_y, core, k) + n * (seq // PARTS), seq // PARTS), :]

    def image_at(chip_x, chip_y, core, k):
        return out.at[pl.ds(rows_of(chip_x, chip_y, core, k), seq), :]

    def put_core(k):
        ref = image_at(x, y, c, k)
        return remote(ref, ref, s_oc, r_oc, cp)

    def pass_y(k):
        ref = image_at(x, 1 - y, c, k)
        return remote(ref, ref, s_ey, r_ey, cp)

    def put(k, n):
        ref = part_of(x, y, c, k, n)
        return (
            remote(ref, ref, s_oy, r_oy.at[k, n], yp),
            remote(ref, ref, s_ox, r_ox.at[k, n], xp),
        )

    def pass_on(k, n):
        of_x = part_of(1 - x, y, c, k, n)
        of_y = part_of(x, 1 - y, c, k, n)
        of_d = part_of(1 - x, 1 - y, c, k, n)
        return (
            remote(of_x, of_x, s_od, r_od.at[k, n], yp),
            remote(of_y, of_y, s_od, r_od.at[k, n], xp),
            remote(of_x, of_x, s_ex, r_ex, cp),
            remote(of_d, of_d, s_ed, r_ed, cp),
        )

    def come(k, n):
        def into(ref, recv):
            return remote(ref, ref, s_ox, recv.at[k, n], cp)

        return (
            into(part_of(1 - x, y, c, k, n), r_ox),
            into(part_of(x, 1 - y, c, k, n), r_oy),
            into(part_of(1 - x, 1 - y, c, k, n), r_od),
        )

    def near_behind(k, when):
        def between(slot):
            @pl.when(when & (slot >= 1))
            def _():
                near(k, slot - 1)

        def rest():
            @pl.when(when)
            def _():
                near(k, CUTS - 1)

        return between, rest

    def near_layer1(k):
        between, rest = near_behind(k + 1, k < OWN - 2)
        rows = pl.ds(pl.multiple_of(rows_of(1 - x, y, c, k), seq), seq)
        layer1(out[rows, :], False, between)
        hid[OWN + k] = acc[0].astype(BF16)
        rest()
        sent(s_g0.at[k], seq)
        for n in range(CUTS):
            part1(k, n, 1 - x).start()

    def far(k, before=None):
        for n in range(CUTS):
            give0(k, n).wait_recv()
        if before is None:
            between, rest = near_behind(OWN - 1, k == 0)
            layer1(x1[k], True, between)
            rest()
        else:
            layer1(x1[k], True)
            before()
        first = rows_of(x, y, c, k)
        for n in range(CUTS):
            part1(k, n, x).wait_recv()
            rows = pl.ds(pl.multiple_of(first + n * (seq // CUTS), seq // CUTS), seq // CUTS)
            out[rows, :] = (acc[0, cut(n), :] + out[rows, :].astype(F32)).astype(BF16)
            for copy in put(k, n):
                copy.start()
        put_core(k).start()

    def pass_x(k, n):
        come(k, n)[0].wait_recv()
        to_d, _, x_core, _ = pass_on(k, n)

        @pl.when(k * PARTS + n < TURN)
        def _():
            to_d.start()

        x_core.start()

    def pass_x_all(k):
        for n in range(PARTS):
            pass_x(k, n)

    near(0, CUTS - 1)
    sent(s_p0.at[0], seq)
    for slot in range(4):
        filled(loc1.at[slot], BLOCK)

    @pl.loop(0, OWN)
    def _(k):
        near_layer1(k)

        @pl.when(k == OWN - 1)
        def _():
            pass_x_all(0)

        @pl.when(k >= 1)
        def _():
            far(k - 1)

    far(OWN - 1, lambda: pass_x_all(1))

    for copy in biases:
        copy.wait_send()
    for sem in (s_c0, s_x0, s_c1, s_y1, s_f1):
        sent(sem, BLOCK)
    for k in range(1, OWN):
        sent(s_p0.at[k], seq)
    sent(s_p1, OWN * seq)

    early, lag = 2, 6
    total = OWN * PARTS

    @pl.loop(0, total + lag)
    def _(j):
        @pl.when(j < total)
        def _():
            k, n = j // PARTS, j % PARTS
            come(k, n)[1].wait_recv()

            @pl.when(j >= TURN)
            def _():
                pass_on(k, n)[1].start()

            @pl.when(n == PARTS - 1)
            def _():
                pass_y(k).start()

        @pl.when((j >= early * PARTS) & (j < total))
        def _():
            pass_x(j // PARTS, j % PARTS)

        @pl.when(j >= lag)
        def _():
            k, n = (j - lag) // PARTS, (j - lag) % PARTS
            come(k, n)[2].wait_recv()
            pass_on(k, n)[3].start()

    for sem in (s_oc, s_ey, s_ox, s_oy, s_od, s_ex, s_ed, r_oc, r_ey, r_ex, r_ed):
        sent(sem, OWN * seq)


def solution(mesh):
    col_spec = P(None, None, "tp")
    row_spec = P(None, "tp", None)
    in_specs = (P("dp", None, None), P(), col_spec, col_spec, col_spec, P(), P(), row_spec, P(), col_spec, P(None, "tp"), row_spec, P())

    def per_device(tokens_in, ln_scale, w_query, w_key, w_value, q_scale, k_scale, w_out, b_out, w_up, b_up, w_down, b_down):
        n_images, seq, dim = tokens_in.shape
        layers, _, heads_w = w_query.shape
        mlp = w_up.shape[2]
        across = lambda w: jnp.swapaxes(w, 1, 2)
        any_spec = pl.BlockSpec(memory_space=pl.ANY)
        vm_spec = pl.BlockSpec(memory_space=pltpu.VMEM)
        dma = lambda *shape: pltpu.SemaphoreType.DMA(shape)
        one = pltpu.SemaphoreType.DMA
        shape = jax.ShapeDtypeStruct
        encoded, *_ = pl.pallas_call(
            fused,
            out_shape=(
                pltpu.VMEM((n_images * seq, dim), BF16),
                shape((3, 3 * heads_w, dim), BF16),
                shape((3, heads_w, dim), BF16),
                shape((3, dim, mlp), BF16),
                shape((3, mlp, dim), BF16),
            ),
            in_specs=[any_spec] * 13,
            out_specs=(vm_spec,) + (any_spec,) * 4,
            scratch_shapes=[
                pltpu.VMEM((4, 3 * heads_w, dim), BF16),
                pltpu.VMEM((4, heads_w, dim), BF16),
                pltpu.VMEM((4, dim, mlp), BF16),
                pltpu.VMEM((4, mlp, dim), BF16),
                pltpu.VMEM((6, layers, mlp), BF16),
                *[pltpu.VMEM(v.shape, BF16) for v in (ln_scale, q_scale, k_scale, b_out, b_down)],
                pltpu.VMEM((layers, 2, q_scale.shape[1], seq), F32),
                pltpu.VMEM((IMGS, seq, dim), F32),
                pltpu.VMEM((IMGS, seq, dim), BF16),
                pltpu.VMEM((OWN, seq, dim), BF16),
                dma(6),
                one, dma(4), dma(IMGS), dma(5), dma(5),
                *[one, dma(PIECES)] * 6,
                *[dma(OWN), dma(OWN, CUTS)] * 2, one, dma(OWN, CUTS),
                *[one] * 4,
                *[one, dma(OWN, PARTS)] * 3,
                *[one] * 4,
            ],
            compiler_params=pltpu.CompilerParams(
                collective_id=0, has_side_effects=True, vmem_limit_bytes=45500000),
        )(tokens_in.reshape(n_images * seq, dim), across(w_query), across(w_key), across(w_value), w_out, w_up, w_down, b_up, ln_scale, q_scale, k_scale, b_out, b_down)
        return encoded.reshape(n_images, seq, dim)

    return jax.shard_map(per_device, mesh=mesh, in_specs=in_specs, out_specs=P("dp", None, None), check_vma=False)
```

```python
import jax
import jax.numpy as jnp
from jax import lax
from jax.experimental import pallas as pl
from jax.experimental.pallas import tpu as pltpu
from jax.sharding import PartitionSpec as P

LN_EPS = 1e-6
MESH = pl.DeviceIdType.MESH
F32, BF16 = jnp.float32, jnp.bfloat16

IMGS = 8
OWN = 4
SPLIT = 384
PIECES = 8
CUTS = 4
PARTS = CUTS
TURN = 15


def normalize(values):
    mean_val = jnp.mean(values, axis=-1, keepdims=True)
    centered = values - mean_val
    variance = jnp.mean(centered * centered, axis=-1, keepdims=True)
    return centered * lax.rsqrt(variance + LN_EPS)


def gelu(pre):
    inner = (2.0 / jnp.pi) ** 0.5 * (pre + 0.044715 * (pre * pre * pre))
    return pre * (0.5 * (1.0 + jnp.tanh(inner)))


def dot(lhs, rhs):
    return jnp.dot(lhs, rhs, preferred_element_type=F32)


def fused(
    tok, wq, wk, wv, wo, w1, w2, bu, ln_in, qs_in, ks_in, bo_in, b2_in,
    out, gq, go, g1, g2,
    vq, vo, v1, v2, vb, ln, qs, ks, bo, b2, gain, acc, hid, x1, s_v,
    loc0, loc1, xs, s_b, r_b,
    s_c0, r_c0, s_x0, r_x0, s_f0, r_f0,
    s_c1, r_c1, s_y1, r_y1, s_f1, r_f1,
    s_p0, r_p0, s_g0, r_g0, s_p1, r_p1,
    s_oc, r_oc, s_ey, r_ey,
    s_ox, r_ox, s_oy, r_oy, s_od, r_od, s_ex, r_ex, s_ed, r_ed,
):
    seq, dim = hid.shape[1], hid.shape[2]
    heads_w = wo.shape[1]
    head_dim = qs.shape[1]
    n_heads = heads_w // head_dim
    mlp = w1.shape[2]
    me = lax.axis_index("tp")
    y = me // 4
    x = (me // 2) % 2
    c = me % 2
    cp = me + 1 - 2 * c
    xp = me + 2 - 4 * x
    yp = me + 4 - 8 * y
    xc = xp + 1 - 2 * c
    yc = yp + 1 - 2 * c

    def remote(src, dst, send, recv, dev):
        return pltpu.make_async_remote_copy(
            src_ref=src, dst_ref=dst, send_sem=send, recv_sem=recv,
            device_id={"tp": dev}, device_id_type=MESH)

    def all_of(sem, rows):
        ref = out.at[pl.ds(0, rows), :]
        return pltpu.make_async_copy(ref, ref, sem)

    def filled(sem, rows):
        all_of(sem, rows).wait()

    sent = filled
    BLOCK = 3 * heads_w + heads_w + 2 * mlp

    def pieces_of(layer):
        return (
            wq.at[layer], wk.at[layer], wv.at[layer], wo.at[layer],
            w1.at[layer, :, pl.ds(0, SPLIT)], w2.at[layer, pl.ds(0, SPLIT), :],
            w1.at[layer, :, pl.ds(SPLIT, mlp - SPLIT)], w2.at[layer, pl.ds(SPLIT, mlp - SPLIT), :],
        )

    def slot_of(refs, slot):
        a, b, d, e = refs
        third = [a.at[slot, pl.ds(n * heads_w, heads_w), :] for n in range(3)]
        return (
            *third, b.at[slot],
            d.at[slot, :, pl.ds(0, SPLIT)], e.at[slot, pl.ds(0, SPLIT), :],
            d.at[slot, :, pl.ds(SPLIT, mlp - SPLIT)], e.at[slot, pl.ds(SPLIT, mlp - SPLIT), :],
        )

    vmem = (vq, vo, v1, v2)
    land = (gq, go, g1, g2)

    def moves(src, dst, send, recv, dev):
        return [remote(src[q], dst[q], send, recv.at[q], dev) for q in range(PIECES)]

    own_load = [pltpu.make_async_copy(pieces_of(0)[q], slot_of(vmem, 0)[q], loc0) for q in range(PIECES)]
    own_core = moves(pieces_of(0), slot_of(vmem, 1), s_c0, r_c0, cp)
    own_x = moves(pieces_of(0), slot_of(vmem, 2), s_x0, r_x0, xp)
    fwd_x = moves(slot_of(vmem, 2), slot_of(vmem, 3), s_f0, r_f0, cp)
    nxt_core = moves(pieces_of(1), slot_of(land, 0), s_c1, r_c1, cp)
    nxt_y = moves(pieces_of(1), slot_of(land, 1), s_y1, r_y1, yp)
    fwd_y = moves(slot_of(land, 1), slot_of(land, 2), s_f1, r_f1, cp)
    peers = (cp, xp, xc, yp, yc)
    biases = [remote(bu, vb.at[n + 1], s_b.at[n], r_b.at[n], peers[n]) for n in range(5)]

    def nxt_load(slot, q):
        src = pieces_of(1) if slot == 0 else slot_of(land, slot - 1)
        return pltpu.make_async_copy(src[q], slot_of(vmem, slot)[q], loc1.at[slot])

    group = (2 * x + c) * IMGS

    def image_of(i):
        far = (i < OWN).astype(jnp.int32) if not isinstance(i, int) else int(i < OWN)
        return group + OWN * (y + far - 2 * y * far) + i % OWN

    def load_x(i):
        return pltpu.make_async_copy(tok.at[pl.ds(image_of(i) * seq, seq), :], hid.at[i], xs.at[i])

    barrier = pltpu.get_barrier_semaphore()
    for dev in peers:
        pl.semaphore_signal(barrier, inc=1, device_id={"tp": dev}, device_id_type=MESH)
    small = [
        pltpu.make_async_copy(src, dst, s_v.at[n])
        for n, (src, dst) in enumerate(
            ((ln_in, ln), (qs_in, qs), (ks_in, ks), (bo_in, bo), (b2_in, b2), (bu, vb.at[0])))
    ]
    for copy in small:
        copy.start()
    for i in range(IMGS):
        load_x(i).start()
    for q in range(PIECES):
        own_load[q].start()
    pl.semaphore_wait(barrier, len(peers))

    for copy in biases:
        copy.start()
    for q in range(PIECES):
        own_x[q].start()
        nxt_y[q].start()
        own_core[q].start()
    for q in range(PIECES):
        nxt_core[q].start()

    def row(ref, layer):
        return ref[layer : layer + 1, :].astype(F32)

    for copy in small:
        copy.wait()
    for layer in range(2):
        for n, ref in enumerate((qs, ks)):
            gain[layer, n] = jnp.broadcast_to(row(ref, layer), (seq, head_dim)).T

    def head_norm(values, layer, n):
        mean_val = jnp.mean(values, axis=0, keepdims=True)
        centered = values - mean_val
        variance = jnp.mean(centered * centered, axis=0, keepdims=True)
        return centered * lax.rsqrt(variance + LN_EPS) * gain[layer, n]

    def heads_of(i, slot):
        return lax.dot_general(vq[slot], hid[i], (((1,), (1,)), ((), ())), preferred_element_type=F32)

    def head_inputs(proj, hd, layer):
        lo = hd * head_dim
        q_h = head_norm(proj[lo : lo + head_dim], layer, 0).astype(BF16)
        k_h = head_norm(proj[heads_w + lo : heads_w + lo + head_dim], layer, 1).astype(BF16).T
        v_h = proj[2 * heads_w + lo : 2 * heads_w + lo + head_dim].astype(BF16)
        return q_h, k_h, v_h

    def softmax(scores):
        scores = scores * head_dim ** -0.5
        weight = jnp.exp(scores - jnp.max(scores, axis=0, keepdims=True))
        total = jnp.sum(weight, axis=0, keepdims=True)
        return (weight * (1.0 / total)).astype(BF16)

    def attend(i, slot, layer):
        proj = heads_of(i, slot)
        parts = [head_inputs(proj, hd, layer) for hd in range(n_heads)]
        scores = [dot(k_h, q_h) for q_h, k_h, _ in parts]
        mixed = [dot(v_h, softmax(sc)) for (_, _, v_h), sc in zip(parts, scores)]
        mix = jnp.concatenate(mixed, axis=0).astype(BF16).T
        return dot(mix, vo[slot])

    def mlp_part(i, slot, layer, lo, hi):
        bias = vb[slot + 2 * layer * (slot // 2), layer : layer + 1, lo:hi].astype(F32)
        act = gelu(dot(hid[i], v1[slot, :, lo:hi]) + bias).astype(BF16)
        return dot(act, v2[slot, lo:hi, :])

    def both(i, slot, layer):
        proj = heads_of(i, slot)
        row_b = vb[slot + 2 * layer * (slot // 2), layer : layer + 1, :].astype(F32)
        bounds = (0, 256, 512, 640)

        def up(n):
            lo, hi = bounds[n], bounds[n + 1]
            return dot(hid[i], v1[slot, :, lo:hi]) + row_b[:, lo:hi]

        def down(n, pre):
            return dot(gelu(pre).astype(BF16), v2[slot, bounds[n] : bounds[n + 1], :])

        pre0 = up(0)
        parts = [head_inputs(proj, hd, layer) for hd in range(n_heads)]
        pre1 = up(1)
        scores = [dot(k_h, q_h) for q_h, k_h, _ in parts]
        pre2 = up(2)
        sum0 = down(0, pre0)
        probs = [softmax(sc) for sc in scores]
        sum1 = down(1, pre1)
        mixed = [dot(v_h, prob) for (_, _, v_h), prob in zip(parts, probs)]
        sum2 = down(2, pre2)
        mix = jnp.concatenate(mixed, axis=0).astype(BF16).T
        return sum0 + sum1 + sum2 + dot(mix, vo[slot])

    @pl.loop(0, IMGS)
    def _(i):
        load_x(i).wait()
        values = hid[i].astype(F32)
        hid[i] = (normalize(values) * row(ln, 0)).astype(BF16)

        @pl.when(i < OWN)
        def _():
            acc[i] = jnp.zeros((seq, dim), F32)

        @pl.when(i >= OWN)
        def _():
            acc[i] = values + row(bo, 0) + row(b2, 0)

    @pl.loop(0, 2)
    def _(slot):
        @pl.when(slot == 0)
        def _():
            filled(loc0, BLOCK)
            for copy in biases:
                copy.wait_recv()

        @pl.when(slot == 1)
        def _():
            for q in range(PIECES):
                own_core[q].wait_recv()

        @pl.loop(0, IMGS)
        def _(i):
            acc[i] += both(i, slot, 0)

    for q in range(PIECES):
        nxt_core[q].wait_recv()
    for q in range(PIECES):
        nxt_load(0, q).start()
        nxt_load(1, q).start()

    def arrive(slot, pieces):
        @pl.when(slot == 2)
        def _():
            for q in pieces:
                own_x[q].wait_recv()
                fwd_x[q].start()

        @pl.when(slot == 3)
        def _():
            for q in pieces:
                fwd_x[q].wait_recv()

    @pl.loop(2, 4)
    def _(slot):
        arrive(slot, (0, 1, 2, 3))

        @pl.loop(0, IMGS)
        def _(i):
            acc[i] += attend(i, slot, 0)

    for q in range(4):
        nxt_y[q].wait_recv()
        fwd_y[q].start()

    @pl.loop(2, 4)
    def _(slot):
        arrive(slot, (4, 5))

        @pl.loop(0, IMGS)
        def _(i):
            acc[i] += mlp_part(i, slot, 0, 0, SPLIT)

    for q in (4, 5):
        nxt_y[q].wait_recv()
        fwd_y[q].start()

    for q in (6, 7):
        own_x[q].wait_recv()
        fwd_x[q].start()
    for q in (6, 7):
        fwd_x[q].wait_recv()

    def cut(n):
        return pl.ds(n * (seq // CUTS), seq // CUTS)

    def rows_of(chip_x, chip_y, core, k):
        return ((2 * (1 - chip_x) + core) * IMGS + OWN * chip_y + k) * seq

    def lent(chip_y, k, n):
        return pl.ds(pl.multiple_of(rows_of(1 - x, chip_y, c, k) + n * (seq // CUTS), seq // CUTS), seq // CUTS)

    def part0(k, n, chip_y):
        return remote(hid.at[k, cut(n), :], out.at[lent(chip_y, k, n), :], s_p0.at[k], r_p0.at[k, n], yp)

    def give0(k, n):
        return remote(out.at[lent(y, k, n), :], x1.at[k, cut(n), :], s_g0.at[k], r_g0.at[k, n], xp)

    def part1(k, n, chip_x):
        rows = pl.ds(pl.multiple_of(rows_of(chip_x, y, c, k) + n * (seq // CUTS), seq // CUTS), seq // CUTS)
        return remote(hid.at[OWN + k, cut(n), :], out.at[rows, :], s_p1, r_p1.at[k, n], xp)

    def near(k, n):
        part0(k, n, y).wait_recv()
        rows = lent(y, k, n)
        out[rows, :] = (acc[OWN + k, cut(n), :] + out[rows, :].astype(F32)).astype(BF16)
        give0(k, n).start()

    @pl.loop(0, OWN)
    def _(k):
        @pl.loop(0, 2)
        def _(mine):
            i = k + OWN * mine
            acc[i] += mlp_part(i, 2, 0, SPLIT, mlp) + mlp_part(i, 3, 0, SPLIT, mlp)

            @pl.when(mine == 0)
            def _():
                hid[k] = acc[k].astype(BF16)
                for n in range(CUTS):
                    part0(k, n, 1 - y).start()

        @pl.when(k == 0)
        def _():
            for q in (6, 7):
                nxt_y[q].wait_recv()
                fwd_y[q].start()

        @pl.when(k >= 1)
        def _():
            near(0, k - 1)

    sent(s_f0, BLOCK)
    for q in range(PIECES):
        nxt_load(2, q).start()
    for q in range(PIECES):
        fwd_y[q].wait_recv()
    for q in range(PIECES):
        nxt_load(3, q).start()

    def part_of(chip_x, chip_y, core, k, n):
        return out.at[pl.ds(rows_of(chip_x, chip_y, core, k) + n * (seq // PARTS), seq // PARTS), :]

    def image_at(chip_x, chip_y, core, k):
        return out.at[pl.ds(rows_of(chip_x, chip_y, core, k), seq), :]

    def put_core(k):
        ref = image_at(x, y, c, k)
        return remote(ref, ref, s_oc, r_oc, cp)

    def pass_y(k):
        ref = image_at(x, 1 - y, c, k)
        return remote(ref, ref, s_ey, r_ey, cp)

    def put(k, n):
        ref = part_of(x, y, c, k, n)
        return (
            remote(ref, ref, s_oy, r_oy.at[k, n], yp),
            remote(ref, ref, s_ox, r_ox.at[k, n], xp),
        )

    def pass_on(k, n):
        of_x = part_of(1 - x, y, c, k, n)
        of_y = part_of(x, 1 - y, c, k, n)
        of_d = part_of(1 - x, 1 - y, c, k, n)
        return (
            remote(of_x, of_x, s_od, r_od.at[k, n], yp),
            remote(of_y, of_y, s_od, r_od.at[k, n], xp),
            remote(of_x, of_x, s_ex, r_ex, cp),
            remote(of_d, of_d, s_ed, r_ed, cp),
        )

    def come(k, n):
        def into(ref, recv):
            return remote(ref, ref, s_ox, recv.at[k, n], cp)

        return (
            into(part_of(1 - x, y, c, k, n), r_ox),
            into(part_of(x, 1 - y, c, k, n), r_oy),
            into(part_of(1 - x, 1 - y, c, k, n), r_od),
        )

    def start_part1(k):
        sent(s_g0.at[k], seq)
        for n in range(CUTS):
            part1(k, n, 1 - x).start()

    def finish(k):
        for n in range(CUTS):
            part1(k, n, x).wait_recv()
            rows = pl.ds(pl.multiple_of(rows_of(x, y, c, k) + n * (seq // CUTS), seq // CUTS), seq // CUTS)
            out[rows, :] = (acc[k, cut(n), :] + out[rows, :].astype(F32)).astype(BF16)
            for copy in put(k, n):
                copy.start()
        put_core(k).start()

    def pass_x(k, n):
        come(k, n)[0].wait_recv()
        to_d, _, x_core, _ = pass_on(k, n)

        @pl.when(k * PARTS + n < TURN)
        def _():
            to_d.start()

        x_core.start()

    def pass_x_all(k):
        for n in range(PARTS):
            pass_x(k, n)

    near(0, CUTS - 1)
    sent(s_p0.at[0], seq)
    for slot in range(4):
        filled(loc1.at[slot], BLOCK)

    @pl.loop(0, 2 * OWN)
    def _(t):
        theirs = (t == 2) | (t == 4) | (t >= 6)
        k_own, k_their = (t + 1) // 2, (t - 1) // 2

        @pl.when(jnp.logical_not(theirs))
        def _():
            values = out[pl.ds(pl.multiple_of(rows_of(1 - x, y, c, k_own), seq), seq), :].astype(F32)
            hid[0] = (normalize(values) * row(ln, 1)).astype(BF16)
            acc[0] = jnp.zeros((seq, dim), F32)

        @pl.when(theirs)
        def _():
            for n in range(CUTS):
                give0(k_their, n).wait_recv()
            values = x1[k_their].astype(F32)
            hid[0] = (normalize(values) * row(ln, 1)).astype(BF16)
            acc[k_their] = values + row(bo, 1) + row(b2, 1)

        where = jnp.where(theirs, k_their, 0)

        @pl.loop(0, 4)
        def _(slot):
            acc[where] += both(0, slot, 1)

            @pl.when((t <= 1) & (slot != 1))
            def _():
                near(t + 1, slot // 2 + slot // 3)

            @pl.when((t == 7) & (slot >= 2))
            def _():
                pass_x(1, slot - 2)

        @pl.when(jnp.logical_not(theirs))
        def _():
            hid[OWN + k_own] = acc[0].astype(BF16)

        @pl.when(t <= 1)
        def _():
            near(t + 1, CUTS - 1)
            start_part1(t)

        @pl.when((t == 2) | (t == 4))
        def _():
            finish(k_their)

        @pl.when(t == 2)
        def _():
            for n in range(CUTS):
                near(OWN - 1, n)

        @pl.when(t == 4)
        def _():
            start_part1(2)

        @pl.when(t == 5)
        def _():
            pass_x_all(0)

        @pl.when(t == 6)
        def _():
            start_part1(3)

    for n in range(2, PARTS):
        pass_x(1, n)
    finish(2)
    finish(3)

    for copy in biases:
        copy.wait_send()
    for sem in (s_c0, s_x0, s_c1, s_y1, s_f1):
        sent(sem, BLOCK)
    for k in range(1, OWN):
        sent(s_p0.at[k], seq)
    sent(s_p1, OWN * seq)

    early, lag = 2, 6
    total = OWN * PARTS

    @pl.loop(0, total + lag)
    def _(j):
        @pl.when(j < total)
        def _():
            k, n = j // PARTS, j % PARTS
            come(k, n)[1].wait_recv()

            @pl.when(j >= TURN)
            def _():
                pass_on(k, n)[1].start()

            @pl.when(n == PARTS - 1)
            def _():
                pass_y(k).start()

        @pl.when((j >= early * PARTS) & (j < total))
        def _():
            pass_x(j // PARTS, j % PARTS)

        @pl.when(j >= lag)
        def _():
            k, n = (j - lag) // PARTS, (j - lag) % PARTS
            come(k, n)[2].wait_recv()
            pass_on(k, n)[3].start()

    for sem in (s_oc, s_ey, s_ox, s_oy, s_od, s_ex, s_ed, r_oc, r_ey, r_ex, r_ed):
        sent(sem, OWN * seq)


def solution(mesh):
    col_spec = P(None, None, "tp")
    row_spec = P(None, "tp", None)
    in_specs = (P("dp", None, None), P(), col_spec, col_spec, col_spec, P(), P(), row_spec, P(), col_spec, P(None, "tp"), row_spec, P())

    def per_device(tokens_in, ln_scale, w_query, w_key, w_value, q_scale, k_scale, w_out, b_out, w_up, b_up, w_down, b_down):
        n_images, seq, dim = tokens_in.shape
        layers, _, heads_w = w_query.shape
        mlp = w_up.shape[2]
        across = lambda w: jnp.swapaxes(w, 1, 2)
        any_spec = pl.BlockSpec(memory_space=pl.ANY)
        vm_spec = pl.BlockSpec(memory_space=pltpu.VMEM)
        dma = lambda *shape: pltpu.SemaphoreType.DMA(shape)
        one = pltpu.SemaphoreType.DMA
        shape = jax.ShapeDtypeStruct
        encoded, *_ = pl.pallas_call(
            fused,
            out_shape=(
                pltpu.VMEM((n_images * seq, dim), BF16),
                shape((3, 3 * heads_w, dim), BF16),
                shape((3, heads_w, dim), BF16),
                shape((3, dim, mlp), BF16),
                shape((3, mlp, dim), BF16),
            ),
            in_specs=[any_spec] * 13,
            out_specs=(vm_spec,) + (any_spec,) * 4,
            scratch_shapes=[
                pltpu.VMEM((4, 3 * heads_w, dim), BF16),
                pltpu.VMEM((4, heads_w, dim), BF16),
                pltpu.VMEM((4, dim, mlp), BF16),
                pltpu.VMEM((4, mlp, dim), BF16),
                pltpu.VMEM((6, layers, mlp), BF16),
                *[pltpu.VMEM(v.shape, BF16) for v in (ln_scale, q_scale, k_scale, b_out, b_down)],
                pltpu.VMEM((layers, 2, q_scale.shape[1], seq), F32),
                pltpu.VMEM((IMGS, seq, dim), F32),
                pltpu.VMEM((IMGS, seq, dim), BF16),
                pltpu.VMEM((OWN, seq, dim), BF16),
                dma(6),
                one, dma(4), dma(IMGS), dma(5), dma(5),
                *[one, dma(PIECES)] * 6,
                *[dma(OWN), dma(OWN, CUTS)] * 2, one, dma(OWN, CUTS),
                *[one] * 4,
                *[one, dma(OWN, PARTS)] * 3,
                *[one] * 4,
            ],
            compiler_params=pltpu.CompilerParams(
                collective_id=0, has_side_effects=True, vmem_limit_bytes=45500000),
        )(tokens_in.reshape(n_images * seq, dim), across(w_query), across(w_key), across(w_value), w_out, w_up, w_down, b_up, ln_scale, q_scale, k_scale, b_out, b_down)
        return encoded.reshape(n_images, seq, dim)

    return jax.shard_map(per_device, mesh=mesh, in_specs=in_specs, out_specs=P("dp", None, None), check_vma=False)
```

```python
import jax
import jax.numpy as jnp
from jax import lax
from jax.experimental import pallas as pl
from jax.experimental.pallas import tpu as pltpu
from jax.sharding import PartitionSpec as P

LN_EPS = 1e-6
MESH = pl.DeviceIdType.MESH
F32, BF16 = jnp.float32, jnp.bfloat16

IMGS = 8
OWN = 4
SPLIT = 384
PIECES = 8
CUTS = 4
PARTS = CUTS
TURN = 15


def normalize(values):
    mean_val = jnp.mean(values, axis=-1, keepdims=True)
    centered = values - mean_val
    variance = jnp.mean(centered * centered, axis=-1, keepdims=True)
    return centered * lax.rsqrt(variance + LN_EPS)


def gelu(pre):
    inner = (2.0 / jnp.pi) ** 0.5 * (pre + 0.044715 * (pre * pre * pre))
    return pre * (0.5 * (1.0 + jnp.tanh(inner)))


def dot(lhs, rhs):
    return jnp.dot(lhs, rhs, preferred_element_type=F32)


def fused(
    tok, wq, wk, wv, wo, w1, w2, bu, ln_in, qs_in, ks_in, bo_in, b2_in,
    out, gq, go, g1, g2,
    vq, vo, v1, v2, vb, ln, qs, ks, bo, b2, gain, acc, hid, x1, s_v,
    loc0, loc1, xs, s_b, r_b,
    s_c0, r_c0, s_x0, r_x0, s_f0, r_f0,
    s_c1, r_c1, s_y1, r_y1, s_f1, r_f1,
    s_p0, r_p0, s_g0, r_g0, s_p1, r_p1,
    s_oc, r_oc, s_ey, r_ey,
    s_ox, r_ox, s_oy, r_oy, s_od, r_od, s_ex, r_ex, s_ed, r_ed,
):
    seq, dim = hid.shape[1], hid.shape[2]
    heads_w = wo.shape[1]
    head_dim = qs.shape[1]
    n_heads = heads_w // head_dim
    mlp = w1.shape[2]
    me = lax.axis_index("tp")
    y = me // 4
    x = (me // 2) % 2
    c = me % 2
    cp = me + 1 - 2 * c
    xp = me + 2 - 4 * x
    yp = me + 4 - 8 * y
    xc = xp + 1 - 2 * c
    yc = yp + 1 - 2 * c

    def remote(src, dst, send, recv, dev):
        return pltpu.make_async_remote_copy(
            src_ref=src, dst_ref=dst, send_sem=send, recv_sem=recv,
            device_id={"tp": dev}, device_id_type=MESH)

    def all_of(sem, rows):
        ref = out.at[pl.ds(0, rows), :]
        return pltpu.make_async_copy(ref, ref, sem)

    def filled(sem, rows):
        all_of(sem, rows).wait()

    sent = filled
    BLOCK = 3 * heads_w + heads_w + 2 * mlp

    def pieces_of(layer):
        return (
            wq.at[layer], wk.at[layer], wv.at[layer], wo.at[layer],
            w1.at[layer, :, pl.ds(0, SPLIT)], w2.at[layer, pl.ds(0, SPLIT), :],
            w1.at[layer, :, pl.ds(SPLIT, mlp - SPLIT)], w2.at[layer, pl.ds(SPLIT, mlp - SPLIT), :],
        )

    def slot_of(refs, slot):
        a, b, d, e = refs
        third = [a.at[slot, pl.ds(n * heads_w, heads_w), :] for n in range(3)]
        return (
            *third, b.at[slot],
            d.at[slot, :, pl.ds(0, SPLIT)], e.at[slot, pl.ds(0, SPLIT), :],
            d.at[slot, :, pl.ds(SPLIT, mlp - SPLIT)], e.at[slot, pl.ds(SPLIT, mlp - SPLIT), :],
        )

    vmem = (vq, vo, v1, v2)
    land = (gq, go, g1, g2)

    def moves(src, dst, send, recv, dev):
        return [remote(src[q], dst[q], send, recv.at[q], dev) for q in range(PIECES)]

    own_load = [pltpu.make_async_copy(pieces_of(0)[q], slot_of(vmem, 0)[q], loc0) for q in range(PIECES)]
    own_core = moves(pieces_of(0), slot_of(vmem, 1), s_c0, r_c0, cp)
    own_x = moves(pieces_of(0), slot_of(vmem, 2), s_x0, r_x0, xp)
    fwd_x = moves(slot_of(vmem, 2), slot_of(vmem, 3), s_f0, r_f0, cp)
    nxt_core = moves(pieces_of(1), slot_of(land, 0), s_c1, r_c1, cp)
    nxt_y = moves(pieces_of(1), slot_of(land, 1), s_y1, r_y1, yp)
    fwd_y = moves(slot_of(land, 1), slot_of(land, 2), s_f1, r_f1, cp)
    peers = (cp, xp, xc, yp, yc)
    biases = [remote(bu, vb.at[n + 1], s_b.at[n], r_b.at[n], peers[n]) for n in range(5)]

    def nxt_load(slot, q):
        src = pieces_of(1) if slot == 0 else slot_of(land, slot - 1)
        return pltpu.make_async_copy(src[q], slot_of(vmem, slot)[q], loc1.at[slot])

    group = (2 * x + c) * IMGS

    def image_of(i):
        far = (i < OWN).astype(jnp.int32) if not isinstance(i, int) else int(i < OWN)
        return group + OWN * (y + far - 2 * y * far) + i % OWN

    def load_x(i):
        return pltpu.make_async_copy(tok.at[pl.ds(image_of(i) * seq, seq), :], hid.at[i], xs.at[i])

    barrier = pltpu.get_barrier_semaphore()
    for dev in peers:
        pl.semaphore_signal(barrier, inc=1, device_id={"tp": dev}, device_id_type=MESH)
    small = [
        pltpu.make_async_copy(src, dst, s_v.at[n])
        for n, (src, dst) in enumerate(
            ((ln_in, ln), (qs_in, qs), (ks_in, ks), (bo_in, bo), (b2_in, b2), (bu, vb.at[0])))
    ]
    for copy in small:
        copy.start()
    for i in range(IMGS):
        load_x(i).start()
    for q in range(PIECES):
        own_load[q].start()
    pl.semaphore_wait(barrier, len(peers))

    for copy in biases:
        copy.start()
    for q in range(PIECES):
        own_x[q].start()
        nxt_y[q].start()
        own_core[q].start()
    for q in range(PIECES):
        nxt_core[q].start()

    def row(ref, layer):
        return ref[layer : layer + 1, :].astype(F32)

    for copy in small:
        copy.wait()
    for layer in range(2):
        for n, ref in enumerate((qs, ks)):
            gain[layer, n] = jnp.broadcast_to(row(ref, layer), (seq, head_dim)).T

    def head_norm(values, layer, n):
        mean_val = jnp.mean(values, axis=0, keepdims=True)
        centered = values - mean_val
        variance = jnp.mean(centered * centered, axis=0, keepdims=True)
        return centered * lax.rsqrt(variance + LN_EPS) * gain[layer, n]

    def heads_of(i, slot):
        return lax.dot_general(vq[slot], hid[i], (((1,), (1,)), ((), ())), preferred_element_type=F32)

    def head_inputs(proj, hd, layer):
        lo = hd * head_dim
        q_h = head_norm(proj[lo : lo + head_dim], layer, 0).astype(BF16)
        k_h = head_norm(proj[heads_w + lo : heads_w + lo + head_dim], layer, 1).astype(BF16).T
        v_h = proj[2 * heads_w + lo : 2 * heads_w + lo + head_dim].astype(BF16)
        return q_h, k_h, v_h

    def softmax(scores):
        scores = scores * head_dim ** -0.5
        weight = jnp.exp(scores - jnp.max(scores, axis=0, keepdims=True))
        total = jnp.sum(weight, axis=0, keepdims=True)
        return (weight * (1.0 / total)).astype(BF16)

    def attend(i, slot, layer):
        proj = heads_of(i, slot)
        parts = [head_inputs(proj, hd, layer) for hd in range(n_heads)]
        scores = [dot(k_h, q_h) for q_h, k_h, _ in parts]
        mixed = [dot(v_h, softmax(sc)) for (_, _, v_h), sc in zip(parts, scores)]
        mix = jnp.concatenate(mixed, axis=0).astype(BF16).T
        return dot(mix, vo[slot])

    def mlp_part(i, slot, layer, lo, hi):
        bias = vb[slot + 2 * layer * (slot // 2), layer : layer + 1, lo:hi].astype(F32)
        act = gelu(dot(hid[i], v1[slot, :, lo:hi]) + bias).astype(BF16)
        return dot(act, v2[slot, lo:hi, :])

    def both(i, slot, layer):
        proj = heads_of(i, slot)
        row_b = vb[slot + 2 * layer * (slot // 2), layer : layer + 1, :].astype(F32)
        bounds = (0, 256, 512, 640)

        def up(n):
            lo, hi = bounds[n], bounds[n + 1]
            return dot(hid[i], v1[slot, :, lo:hi]) + row_b[:, lo:hi]

        def down(n, pre):
            return dot(gelu(pre).astype(BF16), v2[slot, bounds[n] : bounds[n + 1], :])

        pre0 = up(0)
        parts = [head_inputs(proj, hd, layer) for hd in range(n_heads)]
        pre1 = up(1)
        scores = [dot(k_h, q_h) for q_h, k_h, _ in parts]
        pre2 = up(2)
        sum0 = down(0, pre0)
        probs = [softmax(sc) for sc in scores]
        sum1 = down(1, pre1)
        mixed = [dot(v_h, prob) for (_, _, v_h), prob in zip(parts, probs)]
        sum2 = down(2, pre2)
        mix = jnp.concatenate(mixed, axis=0).astype(BF16).T
        return sum0 + sum1 + sum2 + dot(mix, vo[slot])

    @pl.loop(0, IMGS)
    def _(i):
        load_x(i).wait()
        values = hid[i].astype(F32)
        hid[i] = (normalize(values) * row(ln, 0)).astype(BF16)

        @pl.when(i < OWN)
        def _():
            acc[i] = jnp.zeros((seq, dim), F32)

        @pl.when(i >= OWN)
        def _():
            acc[i] = values + row(bo, 0) + row(b2, 0)

    @pl.loop(0, 2)
    def _(slot):
        @pl.when(slot == 0)
        def _():
            filled(loc0, BLOCK)
            for copy in biases:
                copy.wait_recv()

        @pl.when(slot == 1)
        def _():
            for q in range(PIECES):
                own_core[q].wait_recv()

        @pl.loop(0, IMGS)
        def _(i):
            acc[i] += both(i, slot, 0)

    for q in range(PIECES):
        nxt_core[q].wait_recv()
    for q in range(PIECES):
        nxt_load(0, q).start()
        nxt_load(1, q).start()

    def arrive(slot, pieces):
        @pl.when(slot == 2)
        def _():
            for q in pieces:
                own_x[q].wait_recv()
                fwd_x[q].start()

        @pl.when(slot == 3)
        def _():
            for q in pieces:
                fwd_x[q].wait_recv()

    @pl.loop(2, 4)
    def _(slot):
        arrive(slot, (0, 1, 2, 3))

        @pl.loop(0, IMGS)
        def _(i):
            acc[i] += attend(i, slot, 0)

    for q in range(4):
        nxt_y[q].wait_recv()
        fwd_y[q].start()

    @pl.loop(2, 4)
    def _(slot):
        arrive(slot, (4, 5))

        @pl.loop(0, IMGS)
        def _(i):
            acc[i] += mlp_part(i, slot, 0, 0, SPLIT)

    for q in (4, 5):
        nxt_y[q].wait_recv()
        fwd_y[q].start()

    for q in (6, 7):
        own_x[q].wait_recv()
        fwd_x[q].start()
    for q in (6, 7):
        fwd_x[q].wait_recv()

    def cut(n):
        return pl.ds(n * (seq // CUTS), seq // CUTS)

    def rows_of(chip_x, chip_y, core, k):
        return ((2 * (1 - chip_x) + core) * IMGS + OWN * chip_y + k) * seq

    def lent(chip_y, k, n):
        return pl.ds(pl.multiple_of(rows_of(1 - x, chip_y, c, k) + n * (seq // CUTS), seq // CUTS), seq // CUTS)

    def part0(k, n, chip_y):
        return remote(hid.at[k, cut(n), :], out.at[lent(chip_y, k, n), :], s_p0.at[k], r_p0.at[k, n], yp)

    def give0(k, n):
        return remote(out.at[lent(y, k, n), :], x1.at[k, cut(n), :], s_g0.at[k], r_g0.at[k, n], xp)

    def part1(k, n, chip_x):
        rows = pl.ds(pl.multiple_of(rows_of(chip_x, y, c, k) + n * (seq // CUTS), seq // CUTS), seq // CUTS)
        return remote(hid.at[OWN + k, cut(n), :], out.at[rows, :], s_p1, r_p1.at[k, n], xp)

    def near(k, n):
        part0(k, n, y).wait_recv()
        rows = lent(y, k, n)
        out[rows, :] = (acc[OWN + k, cut(n), :] + out[rows, :].astype(F32)).astype(BF16)
        give0(k, n).start()

    @pl.loop(0, OWN)
    def _(k):
        @pl.loop(0, 2)
        def _(mine):
            i = k + OWN * mine
            acc[i] += mlp_part(i, 2, 0, SPLIT, mlp) + mlp_part(i, 3, 0, SPLIT, mlp)

            @pl.when(mine == 0)
            def _():
                hid[k] = acc[k].astype(BF16)
                for n in range(CUTS):
                    part0(k, n, 1 - y).start()

        @pl.when(k == 0)
        def _():
            for q in (6, 7):
                nxt_y[q].wait_recv()
                fwd_y[q].start()

        @pl.when(k >= 1)
        def _():
            near(0, k - 1)

    sent(s_f0, BLOCK)
    for q in range(PIECES):
        nxt_load(2, q).start()
    for q in range(PIECES):
        fwd_y[q].wait_recv()
    for q in range(PIECES):
        nxt_load(3, q).start()

    def part_of(chip_x, chip_y, core, k, n):
        return out.at[pl.ds(rows_of(chip_x, chip_y, core, k) + n * (seq // PARTS), seq // PARTS), :]

    def image_at(chip_x, chip_y, core, k):
        return out.at[pl.ds(rows_of(chip_x, chip_y, core, k), seq), :]

    def put_core(k):
        ref = image_at(x, y, c, k)
        return remote(ref, ref, s_oc, r_oc, cp)

    def pass_y(k):
        ref = image_at(x, 1 - y, c, k)
        return remote(ref, ref, s_ey, r_ey, cp)

    def put(k, n):
        ref = part_of(x, y, c, k, n)
        return (
            remote(ref, ref, s_oy, r_oy.at[k, n], yp),
            remote(ref, ref, s_ox, r_ox.at[k, n], xp),
        )

    def pass_on(k, n):
        of_x = part_of(1 - x, y, c, k, n)
        of_y = part_of(x, 1 - y, c, k, n)
        of_d = part_of(1 - x, 1 - y, c, k, n)
        return (
            remote(of_x, of_x, s_od, r_od.at[k, n], yp),
            remote(of_y, of_y, s_od, r_od.at[k, n], xp),
            remote(of_x, of_x, s_ex, r_ex, cp),
            remote(of_d, of_d, s_ed, r_ed, cp),
        )

    def come(k, n):
        def into(ref, recv):
            return remote(ref, ref, s_ox, recv.at[k, n], cp)

        return (
            into(part_of(1 - x, y, c, k, n), r_ox),
            into(part_of(x, 1 - y, c, k, n), r_oy),
            into(part_of(1 - x, 1 - y, c, k, n), r_od),
        )

    def start_part1(k):
        sent(s_g0.at[k], seq)
        for n in range(CUTS):
            part1(k, n, 1 - x).start()

    def finish_piece(k, n):
        part1(k, n, x).wait_recv()
        rows = pl.ds(pl.multiple_of(rows_of(x, y, c, k) + n * (seq // CUTS), seq // CUTS), seq // CUTS)
        out[rows, :] = (acc[k, cut(n), :] + out[rows, :].astype(F32)).astype(BF16)
        for copy in put(k, n):
            copy.start()

    def finish(k, first=0):
        for n in range(first, CUTS):
            finish_piece(k, n)
        put_core(k).start()

    def pass_x(k, n):
        come(k, n)[0].wait_recv()
        to_d, _, x_core, _ = pass_on(k, n)

        @pl.when(k * PARTS + n < TURN)
        def _():
            to_d.start()

        x_core.start()

    def pass_x_all(k):
        for n in range(PARTS):
            pass_x(k, n)

    near(0, CUTS - 1)
    sent(s_p0.at[0], seq)
    for slot in range(4):
        filled(loc1.at[slot], BLOCK)

    @pl.loop(0, 2 * OWN)
    def _(t):
        theirs = (t == 2) | (t == 4) | (t >= 6)
        k_own, k_their = (t + 1) // 2, (t - 1) // 2

        @pl.when(jnp.logical_not(theirs))
        def _():
            values = out[pl.ds(pl.multiple_of(rows_of(1 - x, y, c, k_own), seq), seq), :].astype(F32)
            hid[0] = (normalize(values) * row(ln, 1)).astype(BF16)
            acc[0] = jnp.zeros((seq, dim), F32)

        @pl.when(theirs)
        def _():
            for n in range(CUTS):
                give0(k_their, n).wait_recv()
            values = x1[k_their].astype(F32)
            hid[0] = (normalize(values) * row(ln, 1)).astype(BF16)
            acc[k_their] = values + row(bo, 1) + row(b2, 1)

        where = jnp.where(theirs, k_their, 0)

        @pl.loop(0, 4)
        def _(slot):
            acc[where] += both(0, slot, 1)

            @pl.when((t <= 1) & (slot != 1))
            def _():
                near(t + 1, slot // 2 + slot // 3)

            @pl.when((t == 7) & (slot % 2 == 1))
            def _():
                finish_piece(2, slot // 2)

        @pl.when(jnp.logical_not(theirs))
        def _():
            hid[OWN + k_own] = acc[0].astype(BF16)

        @pl.when(t <= 1)
        def _():
            near(t + 1, CUTS - 1)
            start_part1(t)

        @pl.when((t == 2) | (t == 4))
        def _():
            finish(k_their)

        @pl.when(t == 4)
        def _():
            for n in range(CUTS):
                near(OWN - 1, n)
            start_part1(2)

        @pl.when(t == 5)
        def _():
            pass_x_all(0)

        @pl.when(t == 6)
        def _():
            pass_x_all(1)
            start_part1(3)

    finish(2, 2)
    finish(3)

    for copy in biases:
        copy.wait_send()
    for sem in (s_c0, s_x0, s_c1, s_y1, s_f1):
        sent(sem, BLOCK)
    for k in range(1, OWN):
        sent(s_p0.at[k], seq)
    sent(s_p1, OWN * seq)

    early, lag = 2, 6
    total = OWN * PARTS

    @pl.loop(0, total + lag)
    def _(j):
        @pl.when(j < total)
        def _():
            k, n = j // PARTS, j % PARTS
            come(k, n)[1].wait_recv()

            @pl.when(j >= TURN)
            def _():
                pass_on(k, n)[1].start()

            @pl.when(n == PARTS - 1)
            def _():
                pass_y(k).start()

        @pl.when((j >= early * PARTS) & (j < total))
        def _():
            pass_x(j // PARTS, j % PARTS)

        @pl.when(j >= lag)
        def _():
            k, n = (j - lag) // PARTS, (j - lag) % PARTS
            come(k, n)[2].wait_recv()
            pass_on(k, n)[3].start()

    for sem in (s_oc, s_ey, s_ox, s_oy, s_od, s_ex, s_ed, r_oc, r_ey, r_ex, r_ed):
        sent(sem, OWN * seq)


def solution(mesh):
    col_spec = P(None, None, "tp")
    row_spec = P(None, "tp", None)
    in_specs = (P("dp", None, None), P(), col_spec, col_spec, col_spec, P(), P(), row_spec, P(), col_spec, P(None, "tp"), row_spec, P())

    def per_device(tokens_in, ln_scale, w_query, w_key, w_value, q_scale, k_scale, w_out, b_out, w_up, b_up, w_down, b_down):
        n_images, seq, dim = tokens_in.shape
        layers, _, heads_w = w_query.shape
        mlp = w_up.shape[2]
        across = lambda w: jnp.swapaxes(w, 1, 2)
        any_spec = pl.BlockSpec(memory_space=pl.ANY)
        vm_spec = pl.BlockSpec(memory_space=pltpu.VMEM)
        dma = lambda *shape: pltpu.SemaphoreType.DMA(shape)
        one = pltpu.SemaphoreType.DMA
        shape = jax.ShapeDtypeStruct
        encoded, *_ = pl.pallas_call(
            fused,
            out_shape=(
                pltpu.VMEM((n_images * seq, dim), BF16),
                shape((3, 3 * heads_w, dim), BF16),
                shape((3, heads_w, dim), BF16),
                shape((3, dim, mlp), BF16),
                shape((3, mlp, dim), BF16),
            ),
            in_specs=[any_spec] * 13,
            out_specs=(vm_spec,) + (any_spec,) * 4,
            scratch_shapes=[
                pltpu.VMEM((4, 3 * heads_w, dim), BF16),
                pltpu.VMEM((4, heads_w, dim), BF16),
                pltpu.VMEM((4, dim, mlp), BF16),
                pltpu.VMEM((4, mlp, dim), BF16),
                pltpu.VMEM((6, layers, mlp), BF16),
                *[pltpu.VMEM(v.shape, BF16) for v in (ln_scale, q_scale, k_scale, b_out, b_down)],
                pltpu.VMEM((layers, 2, q_scale.shape[1], seq), F32),
                pltpu.VMEM((IMGS, seq, dim), F32),
                pltpu.VMEM((IMGS, seq, dim), BF16),
                pltpu.VMEM((OWN, seq, dim), BF16),
                dma(6),
                one, dma(4), dma(IMGS), dma(5), dma(5),
                *[one, dma(PIECES)] * 6,
                *[dma(OWN), dma(OWN, CUTS)] * 2, one, dma(OWN, CUTS),
                *[one] * 4,
                *[one, dma(OWN, PARTS)] * 3,
                *[one] * 4,
            ],
            compiler_params=pltpu.CompilerParams(
                collective_id=0, has_side_effects=True, vmem_limit_bytes=45500000),
        )(tokens_in.reshape(n_images * seq, dim), across(w_query), across(w_key), across(w_value), w_out, w_up, w_down, b_up, ln_scale, q_scale, k_scale, b_out, b_down)
        return encoded.reshape(n_images, seq, dim)

    return jax.shard_map(per_device, mesh=mesh, in_specs=in_specs, out_specs=P("dp", None, None), check_vma=False)
```

```python
import jax
import jax.numpy as jnp
from jax import lax
from jax.experimental import pallas as pl
from jax.experimental.pallas import tpu as pltpu
from jax.sharding import PartitionSpec as P

LN_EPS = 1e-6
MESH = pl.DeviceIdType.MESH
F32, BF16 = jnp.float32, jnp.bfloat16

IMGS = 8
OWN = 4
SPLIT = 384
PIECES = 8
CUTS = 4
PARTS = CUTS
TURN = 15


def normalize(values):
    mean_val = jnp.mean(values, axis=-1, keepdims=True)
    centered = values - mean_val
    variance = jnp.mean(centered * centered, axis=-1, keepdims=True)
    return centered * lax.rsqrt(variance + LN_EPS)


def gelu(pre):
    inner = (2.0 / jnp.pi) ** 0.5 * (pre + 0.044715 * (pre * pre * pre))
    return pre * (0.5 * (1.0 + jnp.tanh(inner)))


def dot(lhs, rhs):
    return jnp.dot(lhs, rhs, preferred_element_type=F32)


def fused(
    tok, wq, wk, wv, wo, w1, w2, bu, ln_in, qs_in, ks_in, bo_in, b2_in,
    out, gq, go, g1, g2,
    vq, vo, v1, v2, vb, ln, qs, ks, bo, b2, gain, acc, hid, x1, s_v,
    loc0, loc1, xs, s_b, r_b,
    s_c0, r_c0, s_x0, r_x0, s_f0, r_f0,
    s_c1, r_c1, s_y1, r_y1, s_f1, r_f1,
    s_p0, r_p0, s_g0, r_g0, s_p1, r_p1,
    s_oc, r_oc, s_ey, r_ey,
    s_ox, r_ox, s_oy, r_oy, s_od, r_od, s_ex, r_ex, s_ed, r_ed,
):
    seq, dim = hid.shape[1], hid.shape[2]
    heads_w = wo.shape[1]
    head_dim = qs.shape[1]
    n_heads = heads_w // head_dim
    mlp = w1.shape[2]
    me = lax.axis_index("tp")
    y = me // 4
    x = (me // 2) % 2
    c = me % 2
    cp = me + 1 - 2 * c
    xp = me + 2 - 4 * x
    yp = me + 4 - 8 * y
    xc = xp + 1 - 2 * c
    yc = yp + 1 - 2 * c

    def remote(src, dst, send, recv, dev):
        return pltpu.make_async_remote_copy(
            src_ref=src, dst_ref=dst, send_sem=send, recv_sem=recv,
            device_id={"tp": dev}, device_id_type=MESH)

    def all_of(sem, rows):
        ref = out.at[pl.ds(0, rows), :]
        return pltpu.make_async_copy(ref, ref, sem)

    def filled(sem, rows):
        all_of(sem, rows).wait()

    sent = filled
    BLOCK = 3 * heads_w + heads_w + 2 * mlp

    def pieces_of(layer):
        return (
            wq.at[layer], wk.at[layer], wv.at[layer], wo.at[layer],
            w1.at[layer, :, pl.ds(0, SPLIT)], w2.at[layer, pl.ds(0, SPLIT), :],
            w1.at[layer, :, pl.ds(SPLIT, mlp - SPLIT)], w2.at[layer, pl.ds(SPLIT, mlp - SPLIT), :],
        )

    def slot_of(refs, slot):
        a, b, d, e = refs
        third = [a.at[slot, pl.ds(n * heads_w, heads_w), :] for n in range(3)]
        return (
            *third, b.at[slot],
            d.at[slot, :, pl.ds(0, SPLIT)], e.at[slot, pl.ds(0, SPLIT), :],
            d.at[slot, :, pl.ds(SPLIT, mlp - SPLIT)], e.at[slot, pl.ds(SPLIT, mlp - SPLIT), :],
        )

    vmem = (vq, vo, v1, v2)
    land = (gq, go, g1, g2)

    def moves(src, dst, send, recv, dev, together=False):
        return [remote(src[q], dst[q], send, recv if together else recv.at[q], dev) for q in range(PIECES)]

    own_load = [pltpu.make_async_copy(pieces_of(0)[q], slot_of(vmem, 0)[q], loc0) for q in range(PIECES)]
    own_core = moves(pieces_of(0), slot_of(vmem, 1), s_c0, r_c0, cp, True)
    own_x = moves(pieces_of(0), slot_of(vmem, 2), s_x0, r_x0, xp)
    fwd_x = moves(slot_of(vmem, 2), slot_of(vmem, 3), s_f0, r_f0, cp)
    nxt_core = moves(pieces_of(1), slot_of(land, 0), s_c1, r_c1, cp, True)
    nxt_y = moves(pieces_of(1), slot_of(land, 1), s_y1, r_y1, yp)
    fwd_y = moves(slot_of(land, 1), slot_of(land, 2), s_f1, r_f1, cp, True)
    peers = (cp, xp, xc, yp, yc)
    biases = [remote(bu, vb.at[n + 1], s_b.at[n], r_b.at[n], peers[n]) for n in range(5)]

    def nxt_load(slot, q):
        src = pieces_of(1) if slot == 0 else slot_of(land, slot - 1)
        return pltpu.make_async_copy(src[q], slot_of(vmem, slot)[q], loc1.at[slot])

    group = (2 * x + c) * IMGS

    def image_of(i):
        far = (i < OWN).astype(jnp.int32) if not isinstance(i, int) else int(i < OWN)
        return group + OWN * (y + far - 2 * y * far) + i % OWN

    def load_x(i):
        return pltpu.make_async_copy(tok.at[pl.ds(image_of(i) * seq, seq), :], hid.at[i], xs.at[i])

    barrier = pltpu.get_barrier_semaphore()
    for dev in peers:
        pl.semaphore_signal(barrier, inc=1, device_id={"tp": dev}, device_id_type=MESH)
    small = [
        pltpu.make_async_copy(src, dst, s_v.at[n])
        for n, (src, dst) in enumerate(
            ((ln_in, ln), (qs_in, qs), (ks_in, ks), (bo_in, bo), (b2_in, b2), (bu, vb.at[0])))
    ]
    for copy in small:
        copy.start()
    for i in range(IMGS):
        load_x(i).start()
    for q in range(PIECES):
        own_load[q].start()
    pl.semaphore_wait(barrier, len(peers))

    for q in range(PIECES):
        own_x[q].start()
        nxt_y[q].start()
        if q == 3:
            for copy in biases:
                copy.start()
        own_core[q].start()
    for q in range(PIECES):
        nxt_core[q].start()

    def row(ref, layer):
        return ref[layer : layer + 1, :].astype(F32)

    for copy in small:
        copy.wait()
    for layer in range(2):
        for n, ref in enumerate((qs, ks)):
            gain[layer, n] = jnp.broadcast_to(row(ref, layer), (seq, head_dim)).T

    def head_norm(values, layer, n):
        mean_val = jnp.mean(values, axis=0, keepdims=True)
        centered = values - mean_val
        variance = jnp.mean(centered * centered, axis=0, keepdims=True)
        return centered * lax.rsqrt(variance + LN_EPS) * gain[layer, n]

    def heads_of(i, slot):
        return lax.dot_general(vq[slot], hid[i], (((1,), (1,)), ((), ())), preferred_element_type=F32)

    def head_inputs(proj, hd, layer):
        lo = hd * head_dim
        q_h = head_norm(proj[lo : lo + head_dim], layer, 0).astype(BF16)
        k_h = head_norm(proj[heads_w + lo : heads_w + lo + head_dim], layer, 1).astype(BF16).T
        v_h = proj[2 * heads_w + lo : 2 * heads_w + lo + head_dim].astype(BF16)
        return q_h, k_h, v_h

    def softmax(scores):
        scores = scores * head_dim ** -0.5
        weight = jnp.exp(scores - jnp.max(scores, axis=0, keepdims=True))
        total = jnp.sum(weight, axis=0, keepdims=True)
        return (weight * (1.0 / total)).astype(BF16)

    def attend(i, slot, layer):
        proj = heads_of(i, slot)
        parts = [head_inputs(proj, hd, layer) for hd in range(n_heads)]
        scores = [dot(k_h, q_h) for q_h, k_h, _ in parts]
        mixed = [dot(v_h, softmax(sc)) for (_, _, v_h), sc in zip(parts, scores)]
        mix = jnp.concatenate(mixed, axis=0).astype(BF16).T
        return dot(mix, vo[slot])

    def mlp_part(i, slot, layer, lo, hi):
        bias = vb[slot + 2 * layer * (slot // 2), layer : layer + 1, lo:hi].astype(F32)
        act = gelu(dot(hid[i], v1[slot, :, lo:hi]) + bias).astype(BF16)
        return dot(act, v2[slot, lo:hi, :])

    def both(i, slot, layer):
        proj = heads_of(i, slot)
        row_b = vb[slot + 2 * layer * (slot // 2), layer : layer + 1, :].astype(F32)
        bounds = (0, 256, 512, 640)

        def up(n):
            lo, hi = bounds[n], bounds[n + 1]
            return dot(hid[i], v1[slot, :, lo:hi]) + row_b[:, lo:hi]

        def down(n, pre):
            return dot(gelu(pre).astype(BF16), v2[slot, bounds[n] : bounds[n + 1], :])

        pre0 = up(0)
        parts = [head_inputs(proj, hd, layer) for hd in range(n_heads)]
        pre1 = up(1)
        scores = [dot(k_h, q_h) for q_h, k_h, _ in parts]
        pre2 = up(2)
        sum0 = down(0, pre0)
        probs = [softmax(sc) for sc in scores]
        sum1 = down(1, pre1)
        mixed = [dot(v_h, prob) for (_, _, v_h), prob in zip(parts, probs)]
        sum2 = down(2, pre2)
        mix = jnp.concatenate(mixed, axis=0).astype(BF16).T
        return sum0 + sum1 + sum2 + dot(mix, vo[slot])

    @pl.loop(0, IMGS)
    def _(i):
        load_x(i).wait()
        values = hid[i].astype(F32)
        hid[i] = (normalize(values) * row(ln, 0)).astype(BF16)

        @pl.when(i < OWN)
        def _():
            acc[i] = jnp.zeros((seq, dim), F32)

        @pl.when(i >= OWN)
        def _():
            acc[i] = values + row(bo, 0) + row(b2, 0)

    @pl.loop(0, 2)
    def _(slot):
        @pl.when(slot == 0)
        def _():
            filled(loc0, BLOCK)

        @pl.when(slot == 1)
        def _():
            biases[0].wait_recv()
            filled(r_c0, BLOCK)

        @pl.loop(0, IMGS)
        def _(i):
            acc[i] += both(i, slot, 0)

    filled(r_c1, BLOCK)
    for q in range(PIECES):
        nxt_load(0, q).start()
        nxt_load(1, q).start()

    for copy in biases[1:]:
        copy.wait_recv()

    def arrive(slot, pieces):
        @pl.when(slot == 2)
        def _():
            for q in pieces:
                own_x[q].wait_recv()
                fwd_x[q].start()

        @pl.when(slot == 3)
        def _():
            for q in pieces:
                fwd_x[q].wait_recv()

    @pl.loop(2, 4)
    def _(slot):
        arrive(slot, (0, 1, 2, 3))

        @pl.loop(0, IMGS)
        def _(i):
            acc[i] += attend(i, slot, 0)

    for q in range(4):
        nxt_y[q].wait_recv()
        fwd_y[q].start()

    @pl.loop(2, 4)
    def _(slot):
        arrive(slot, (4, 5))

        @pl.loop(0, IMGS)
        def _(i):
            acc[i] += mlp_part(i, slot, 0, 0, SPLIT)

    for q in (4, 5):
        nxt_y[q].wait_recv()
        fwd_y[q].start()

    for q in (6, 7):
        own_x[q].wait_recv()
        fwd_x[q].start()

    @pl.loop(0, 2)
    def _(mine):
        acc[OWN * mine] += mlp_part(OWN * mine, 2, 0, SPLIT, mlp)

    for q in (6, 7):
        fwd_x[q].wait_recv()

    def cut(n):
        return pl.ds(n * (seq // CUTS), seq // CUTS)

    def rows_of(chip_x, chip_y, core, k):
        return ((2 * (1 - chip_x) + core) * IMGS + OWN * chip_y + k) * seq

    def lent(chip_y, k, n):
        return pl.ds(pl.multiple_of(rows_of(1 - x, chip_y, c, k) + n * (seq // CUTS), seq // CUTS), seq // CUTS)

    def part0(k, n, chip_y):
        return remote(hid.at[k, cut(n), :], out.at[lent(chip_y, k, n), :], s_p0.at[k], r_p0.at[k, n], yp)

    def give0(k, n):
        return remote(out.at[lent(y, k, n), :], x1.at[k, cut(n), :], s_g0.at[k], r_g0.at[k, n], xp)

    def part1(k, n, chip_x):
        rows = pl.ds(pl.multiple_of(rows_of(chip_x, y, c, k) + n * (seq // CUTS), seq // CUTS), seq // CUTS)
        return remote(hid.at[OWN + k, cut(n), :], out.at[rows, :], s_p1, r_p1.at[k, n], xp)

    def near(k, n):
        part0(k, n, y).wait_recv()
        rows = lent(y, k, n)
        out[rows, :] = (acc[OWN + k, cut(n), :] + out[rows, :].astype(F32)).astype(BF16)
        give0(k, n).start()

    @pl.loop(0, OWN)
    def _(k):
        @pl.loop(0, 2)
        def _(mine):
            i = k + OWN * mine

            @pl.when(k == 0)
            def _():
                acc[i] += mlp_part(i, 3, 0, SPLIT, mlp)

            @pl.when(k > 0)
            def _():
                acc[i] += mlp_part(i, 2, 0, SPLIT, mlp) + mlp_part(i, 3, 0, SPLIT, mlp)

            @pl.when(mine == 0)
            def _():
                hid[k] = acc[k].astype(BF16)
                for n in range(CUTS):
                    part0(k, n, 1 - y).start()

        @pl.when(k == 0)
        def _():
            for q in (6, 7):
                nxt_y[q].wait_recv()
                fwd_y[q].start()

        @pl.when(k >= 1)
        def _():
            near(0, k - 1)

    sent(s_f0, BLOCK)
    for q in range(PIECES):
        nxt_load(2, q).start()
    filled(r_f1, BLOCK)
    for q in range(PIECES):
        nxt_load(3, q).start()

    def part_of(chip_x, chip_y, core, k, n):
        return out.at[pl.ds(rows_of(chip_x, chip_y, core, k) + n * (seq // PARTS), seq // PARTS), :]

    def image_at(chip_x, chip_y, core, k):
        return out.at[pl.ds(rows_of(chip_x, chip_y, core, k), seq), :]

    def put_core(k):
        ref = image_at(x, y, c, k)
        return remote(ref, ref, s_oc, r_oc, cp)

    def pass_y(k):
        ref = image_at(x, 1 - y, c, k)
        return remote(ref, ref, s_ey, r_ey, cp)

    def put(k, n):
        ref = part_of(x, y, c, k, n)
        return (
            remote(ref, ref, s_oy, r_oy.at[k, n], yp),
            remote(ref, ref, s_ox, r_ox.at[k, n], xp),
        )

    def pass_on(k, n):
        of_x = part_of(1 - x, y, c, k, n)
        of_y = part_of(x, 1 - y, c, k, n)
        of_d = part_of(1 - x, 1 - y, c, k, n)
        return (
            remote(of_x, of_x, s_od, r_od.at[k, n], yp),
            remote(of_y, of_y, s_od, r_od.at[k, n], xp),
            remote(of_x, of_x, s_ex, r_ex, cp),
            remote(of_d, of_d, s_ed, r_ed, cp),
        )

    def come(k, n):
        def into(ref, recv):
            return remote(ref, ref, s_ox, recv.at[k, n], cp)

        return (
            into(part_of(1 - x, y, c, k, n), r_ox),
            into(part_of(x, 1 - y, c, k, n), r_oy),
            into(part_of(1 - x, 1 - y, c, k, n), r_od),
        )

    def start_part1(k):
        sent(s_g0.at[k], seq)
        for n in range(CUTS):
            part1(k, n, 1 - x).start()

    def finish_piece(k, n):
        part1(k, n, x).wait_recv()
        rows = pl.ds(pl.multiple_of(rows_of(x, y, c, k) + n * (seq // CUTS), seq // CUTS), seq // CUTS)
        out[rows, :] = (acc[k, cut(n), :] + out[rows, :].astype(F32)).astype(BF16)
        for copy in put(k, n):
            copy.start()

    def finish(k, first=0):
        for n in range(first, CUTS):
            finish_piece(k, n)
        put_core(k).start()

    def pass_x(k, n):
        come(k, n)[0].wait_recv()
        to_d, _, x_core, _ = pass_on(k, n)

        @pl.when(k * PARTS + n < TURN)
        def _():
            to_d.start()

        x_core.start()

    def pass_x_all(k):
        for n in range(PARTS):
            pass_x(k, n)

    near(0, CUTS - 1)
    sent(s_p0.at[0], seq)
    for slot in range(4):
        filled(loc1.at[slot], BLOCK)

    @pl.loop(0, 2 * OWN)
    def _(t):
        theirs = (t == 2) | (t == 4) | (t >= 6)
        k_own, k_their = (t + 1) // 2, (t - 1) // 2

        @pl.when(jnp.logical_not(theirs))
        def _():
            values = out[pl.ds(pl.multiple_of(rows_of(1 - x, y, c, k_own), seq), seq), :].astype(F32)
            hid[0] = (normalize(values) * row(ln, 1)).astype(BF16)
            acc[0] = jnp.zeros((seq, dim), F32)

        @pl.when(theirs)
        def _():
            for n in range(CUTS):
                give0(k_their, n).wait_recv()
            values = x1[k_their].astype(F32)
            hid[0] = (normalize(values) * row(ln, 1)).astype(BF16)
            acc[k_their] = values + row(bo, 1) + row(b2, 1)

        where = jnp.where(theirs, k_their, 0)

        @pl.loop(0, 4)
        def _(slot):
            acc[where] += both(0, slot, 1)

            @pl.when((t <= 1) & (slot != 1))
            def _():
                near(t + 1, slot // 2 + slot // 3)

            @pl.when((t == 7) & (slot % 2 == 1))
            def _():
                finish_piece(2, slot // 2)

        @pl.when(jnp.logical_not(theirs))
        def _():
            hid[OWN + k_own] = acc[0].astype(BF16)

        @pl.when(t <= 1)
        def _():
            near(t + 1, CUTS - 1)
            start_part1(t)

        @pl.when((t == 2) | (t == 4))
        def _():
            finish(k_their)

        @pl.when(t == 4)
        def _():
            for n in range(CUTS):
                near(OWN - 1, n)
            start_part1(2)

        @pl.when(t == 5)
        def _():
            pass_x_all(0)

        @pl.when(t == 6)
        def _():
            pass_x_all(1)
            start_part1(3)

    finish(2, 2)
    finish(3)

    for copy in biases:
        copy.wait_send()
    for sem in (s_c0, s_x0, s_c1, s_y1, s_f1):
        sent(sem, BLOCK)
    for k in range(1, OWN):
        sent(s_p0.at[k], seq)
    sent(s_p1, OWN * seq)

    early, lag = 2, 6
    total = OWN * PARTS

    @pl.loop(0, total + lag)
    def _(j):
        @pl.when(j < total)
        def _():
            k, n = j // PARTS, j % PARTS
            come(k, n)[1].wait_recv()

            @pl.when(j >= TURN)
            def _():
                pass_on(k, n)[1].start()

            @pl.when(n == PARTS - 1)
            def _():
                pass_y(k).start()

        @pl.when((j >= early * PARTS) & (j < total))
        def _():
            pass_x(j // PARTS, j % PARTS)

        @pl.when(j >= lag)
        def _():
            k, n = (j - lag) // PARTS, (j - lag) % PARTS
            come(k, n)[2].wait_recv()
            pass_on(k, n)[3].start()

    for sem in (s_oc, s_ey, s_ox, s_oy, s_od, s_ex, s_ed, r_oc, r_ey, r_ex, r_ed):
        sent(sem, OWN * seq)


def solution(mesh):
    col_spec = P(None, None, "tp")
    row_spec = P(None, "tp", None)
    in_specs = (P("dp", None, None), P(), col_spec, col_spec, col_spec, P(), P(), row_spec, P(), col_spec, P(None, "tp"), row_spec, P())

    def per_device(tokens_in, ln_scale, w_query, w_key, w_value, q_scale, k_scale, w_out, b_out, w_up, b_up, w_down, b_down):
        n_images, seq, dim = tokens_in.shape
        layers, _, heads_w = w_query.shape
        mlp = w_up.shape[2]
        across = lambda w: jnp.swapaxes(w, 1, 2)
        any_spec = pl.BlockSpec(memory_space=pl.ANY)
        vm_spec = pl.BlockSpec(memory_space=pltpu.VMEM)
        dma = lambda *shape: pltpu.SemaphoreType.DMA(shape)
        one = pltpu.SemaphoreType.DMA
        shape = jax.ShapeDtypeStruct
        encoded, *_ = pl.pallas_call(
            fused,
            out_shape=(
                pltpu.VMEM((n_images * seq, dim), BF16),
                shape((3, 3 * heads_w, dim), BF16),
                shape((3, heads_w, dim), BF16),
                shape((3, dim, mlp), BF16),
                shape((3, mlp, dim), BF16),
            ),
            in_specs=[any_spec] * 13,
            out_specs=(vm_spec,) + (any_spec,) * 4,
            scratch_shapes=[
                pltpu.VMEM((4, 3 * heads_w, dim), BF16),
                pltpu.VMEM((4, heads_w, dim), BF16),
                pltpu.VMEM((4, dim, mlp), BF16),
                pltpu.VMEM((4, mlp, dim), BF16),
                pltpu.VMEM((6, layers, mlp), BF16),
                *[pltpu.VMEM(v.shape, BF16) for v in (ln_scale, q_scale, k_scale, b_out, b_down)],
                pltpu.VMEM((layers, 2, q_scale.shape[1], seq), F32),
                pltpu.VMEM((IMGS, seq, dim), F32),
                pltpu.VMEM((IMGS, seq, dim), BF16),
                pltpu.VMEM((OWN, seq, dim), BF16),
                dma(6),
                one, dma(4), dma(IMGS), dma(5), dma(5),
                one, one, *[one, dma(PIECES)] * 2,
                one, one, one, dma(PIECES), one, one,
                *[dma(OWN), dma(OWN, CUTS)] * 2, one, dma(OWN, CUTS),
                *[one] * 4,
                *[one, dma(OWN, PARTS)] * 3,
                *[one] * 4,
            ],
            compiler_params=pltpu.CompilerParams(
                collective_id=0, has_side_effects=True, vmem_limit_bytes=45500000),
        )(tokens_in.reshape(n_images * seq, dim), across(w_query), across(w_key), across(w_value), w_out, w_up, w_down, b_up, ln_scale, q_scale, k_scale, b_out, b_down)
        return encoded.reshape(n_images, seq, dim)

    return jax.shard_map(per_device, mesh=mesh, in_specs=in_specs, out_specs=P("dp", None, None), check_vma=False)
```

```python
import jax
import jax.numpy as jnp
from jax import lax
from jax.experimental import pallas as pl
from jax.experimental.pallas import tpu as pltpu
from jax.sharding import PartitionSpec as P

LN_EPS = 1e-6
MESH = pl.DeviceIdType.MESH
F32, BF16 = jnp.float32, jnp.bfloat16

IMGS = 8
OWN = 4
SPLIT = 384
PIECES = 8
CUTS = 4
PARTS = CUTS
TURN = 15


def normalize(values):
    mean_val = jnp.mean(values, axis=-1, keepdims=True)
    centered = values - mean_val
    variance = jnp.mean(centered * centered, axis=-1, keepdims=True)
    return centered * lax.rsqrt(variance + LN_EPS)


def gelu(pre):
    inner = (2.0 / jnp.pi) ** 0.5 * (pre + 0.044715 * (pre * pre * pre))
    return pre * (0.5 * (1.0 + jnp.tanh(inner)))


def dot(lhs, rhs):
    return jnp.dot(lhs, rhs, preferred_element_type=F32)


def fused(
    tok, wq, wk, wv, wo, w1, w2, bu, ln_in, qs_in, ks_in, bo_in, b2_in,
    out, gq, go, g1, g2,
    vq, vo, v1, v2, vb, ln, qs, ks, bo, b2, gain, acc, hid, x1, s_v,
    loc0, loc1, xs, s_b, r_b,
    s_c0, r_c0, s_x0, r_x0, s_f0, r_f0,
    s_c1, r_c1, s_y1, r_y1, s_f1, r_f1,
    s_p0, r_p0, s_g0, r_g0, s_p1, r_p1,
    s_oc, r_oc, s_ey, r_ey,
    s_ox, r_ox, s_oy, r_oy, s_od, r_od, s_ex, r_ex, s_ed, r_ed,
):
    seq, dim = hid.shape[1], hid.shape[2]
    heads_w = wo.shape[1]
    head_dim = qs.shape[1]
    n_heads = heads_w // head_dim
    mlp = w1.shape[2]
    me = lax.axis_index("tp")
    y = me // 4
    x = (me // 2) % 2
    c = me % 2
    cp = me + 1 - 2 * c
    xp = me + 2 - 4 * x
    yp = me + 4 - 8 * y
    xc = xp + 1 - 2 * c
    yc = yp + 1 - 2 * c

    def remote(src, dst, send, recv, dev):
        return pltpu.make_async_remote_copy(
            src_ref=src, dst_ref=dst, send_sem=send, recv_sem=recv,
            device_id={"tp": dev}, device_id_type=MESH)

    def all_of(sem, rows):
        ref = out.at[pl.ds(0, rows), :]
        return pltpu.make_async_copy(ref, ref, sem)

    def filled(sem, rows):
        all_of(sem, rows).wait()

    sent = filled
    BLOCK = 3 * heads_w + heads_w + 2 * mlp

    def pieces_of(layer):
        return (
            wq.at[layer], wk.at[layer], wv.at[layer], wo.at[layer],
            w1.at[layer, :, pl.ds(0, SPLIT)], w2.at[layer, pl.ds(0, SPLIT), :],
            w1.at[layer, :, pl.ds(SPLIT, mlp - SPLIT)], w2.at[layer, pl.ds(SPLIT, mlp - SPLIT), :],
        )

    def slot_of(refs, slot):
        a, b, d, e = refs
        third = [a.at[slot, pl.ds(n * heads_w, heads_w), :] for n in range(3)]
        return (
            *third, b.at[slot],
            d.at[slot, :, pl.ds(0, SPLIT)], e.at[slot, pl.ds(0, SPLIT), :],
            d.at[slot, :, pl.ds(SPLIT, mlp - SPLIT)], e.at[slot, pl.ds(SPLIT, mlp - SPLIT), :],
        )

    vmem = (vq, vo, v1, v2)
    land = (gq, go, g1, g2)

    def moves(src, dst, send, recv, dev, together=False):
        return [remote(src[q], dst[q], send, recv if together else recv.at[q], dev) for q in range(PIECES)]

    own_load = [pltpu.make_async_copy(pieces_of(0)[q], slot_of(vmem, 0)[q], loc0) for q in range(PIECES)]
    own_core = moves(pieces_of(0), slot_of(vmem, 1), s_c0, r_c0, cp, True)
    own_x = moves(pieces_of(0), slot_of(vmem, 2), s_x0, r_x0, xp)
    fwd_x = moves(slot_of(vmem, 2), slot_of(vmem, 3), s_f0, r_f0, cp)
    nxt_core = moves(pieces_of(1), slot_of(land, 0), s_c1, r_c1, cp, True)
    nxt_y = moves(pieces_of(1), slot_of(land, 1), s_y1, r_y1, yp)
    fwd_y = moves(slot_of(land, 1), slot_of(land, 2), s_f1, r_f1, cp, True)
    peers = (cp, xp, xc, yp, yc)
    biases = [remote(bu, vb.at[n + 1], s_b.at[n], r_b.at[n], peers[n]) for n in range(5)]

    def nxt_load(slot, q):
        src = pieces_of(1) if slot == 0 else slot_of(land, slot - 1)
        return pltpu.make_async_copy(src[q], slot_of(vmem, slot)[q], loc1.at[slot])

    group = (2 * x + c) * IMGS

    def image_of(i):
        far = (i < OWN).astype(jnp.int32) if not isinstance(i, int) else int(i < OWN)
        return group + OWN * (y + far - 2 * y * far) + i % OWN

    def load_x(i):
        return pltpu.make_async_copy(tok.at[pl.ds(image_of(i) * seq, seq), :], hid.at[i], xs.at[i])

    barrier = pltpu.get_barrier_semaphore()
    for dev in peers:
        pl.semaphore_signal(barrier, inc=1, device_id={"tp": dev}, device_id_type=MESH)
    small = [
        pltpu.make_async_copy(src, dst, s_v.at[n])
        for n, (src, dst) in enumerate(
            ((ln_in, ln), (qs_in, qs), (ks_in, ks), (bo_in, bo), (b2_in, b2), (bu, vb.at[0])))
    ]
    for copy in small:
        copy.start()
    for i in range(IMGS):
        load_x(i).start()
    for q in range(PIECES):
        own_load[q].start()
    pl.semaphore_wait(barrier, len(peers))

    for q in range(PIECES):
        own_x[q].start()
        nxt_y[q].start()
        if q == 3:
            for copy in biases:
                copy.start()
        own_core[q].start()
    for q in range(PIECES):
        nxt_core[q].start()

    def row(ref, layer):
        return ref[layer : layer + 1, :].astype(F32)

    for copy in small:
        copy.wait()
    for layer in range(2):
        for n, ref in enumerate((qs, ks)):
            gain[layer, n] = jnp.broadcast_to(row(ref, layer), (seq, head_dim)).T

    def head_norm(values, layer, n):
        mean_val = jnp.mean(values, axis=0, keepdims=True)
        centered = values - mean_val
        variance = jnp.mean(centered * centered, axis=0, keepdims=True)
        return centered * lax.rsqrt(variance + LN_EPS) * gain[layer, n]

    def heads_of(i, slot):
        return lax.dot_general(vq[slot], hid[i], (((1,), (1,)), ((), ())), preferred_element_type=F32)

    def head_inputs(proj, hd, layer):
        lo = hd * head_dim
        q_h = head_norm(proj[lo : lo + head_dim], layer, 0).astype(BF16)
        k_h = head_norm(proj[heads_w + lo : heads_w + lo + head_dim], layer, 1).astype(BF16).T
        v_h = proj[2 * heads_w + lo : 2 * heads_w + lo + head_dim].astype(BF16)
        return q_h, k_h, v_h

    def softmax(scores):
        scores = scores * head_dim ** -0.5
        weight = jnp.exp(scores - jnp.max(scores, axis=0, keepdims=True))
        total = jnp.sum(weight, axis=0, keepdims=True)
        return (weight * (1.0 / total)).astype(BF16)

    def attend(i, slot, layer):
        proj = heads_of(i, slot)
        parts = [head_inputs(proj, hd, layer) for hd in range(n_heads)]
        scores = [dot(k_h, q_h) for q_h, k_h, _ in parts]
        mixed = [dot(v_h, softmax(sc)) for (_, _, v_h), sc in zip(parts, scores)]
        mix = jnp.concatenate(mixed, axis=0).astype(BF16).T
        return dot(mix, vo[slot])

    def mlp_part(i, slot, layer, lo, hi):
        bias = vb[slot + 2 * layer * (slot // 2), layer : layer + 1, lo:hi].astype(F32)
        act = gelu(dot(hid[i], v1[slot, :, lo:hi]) + bias).astype(BF16)
        return dot(act, v2[slot, lo:hi, :])

    def both(i, slot, layer):
        proj = heads_of(i, slot)
        row_b = vb[slot + 2 * layer * (slot // 2), layer : layer + 1, :].astype(F32)
        bounds = (0, 256, 512, 640)

        def up(n):
            lo, hi = bounds[n], bounds[n + 1]
            return dot(hid[i], v1[slot, :, lo:hi]) + row_b[:, lo:hi]

        def down(n, pre):
            return dot(gelu(pre).astype(BF16), v2[slot, bounds[n] : bounds[n + 1], :])

        pre0 = up(0)
        parts = [head_inputs(proj, hd, layer) for hd in range(n_heads)]
        pre1 = up(1)
        scores = [dot(k_h, q_h) for q_h, k_h, _ in parts]
        pre2 = up(2)
        sum0 = down(0, pre0)
        probs = [softmax(sc) for sc in scores]
        sum1 = down(1, pre1)
        mixed = [dot(v_h, prob) for (_, _, v_h), prob in zip(parts, probs)]
        sum2 = down(2, pre2)
        mix = jnp.concatenate(mixed, axis=0).astype(BF16).T
        return sum0 + sum1 + sum2 + dot(mix, vo[slot])

    @pl.loop(0, IMGS)
    def _(i):
        load_x(i).wait()
        values = hid[i].astype(F32)
        hid[i] = (normalize(values) * row(ln, 0)).astype(BF16)

        @pl.when(i < OWN)
        def _():
            acc[i] = jnp.zeros((seq, dim), F32)

        @pl.when(i >= OWN)
        def _():
            acc[i] = values + row(bo, 0) + row(b2, 0)

    @pl.loop(0, 2)
    def _(slot):
        @pl.when(slot == 0)
        def _():
            filled(loc0, BLOCK)

        @pl.when(slot == 1)
        def _():
            biases[0].wait_recv()
            filled(r_c0, BLOCK)

        @pl.loop(0, IMGS)
        def _(i):
            acc[i] += both(i, slot, 0)

    filled(r_c1, BLOCK)
    for q in range(PIECES):
        nxt_load(0, q).start()
        nxt_load(1, q).start()

    for copy in biases[1:]:
        copy.wait_recv()

    def arrive(slot, pieces):
        @pl.when(slot == 2)
        def _():
            for q in pieces:
                own_x[q].wait_recv()
                fwd_x[q].start()

        @pl.when(slot == 3)
        def _():
            for q in pieces:
                fwd_x[q].wait_recv()

    @pl.loop(2, 4)
    def _(slot):
        arrive(slot, (0, 1, 2, 3))

        @pl.loop(0, IMGS)
        def _(i):
            acc[i] += attend(i, slot, 0)

    for q in range(4):
        nxt_y[q].wait_recv()
        fwd_y[q].start()

    @pl.loop(2, 4)
    def _(slot):
        arrive(slot, (4, 5))

        @pl.loop(0, IMGS)
        def _(i):
            acc[i] += mlp_part(i, slot, 0, 0, SPLIT)

    for q in (4, 5):
        nxt_y[q].wait_recv()
        fwd_y[q].start()

    for q in (6, 7):
        own_x[q].wait_recv()
        fwd_x[q].start()

    acc[0] += mlp_part(0, 2, 0, SPLIT, mlp)

    for q in (6, 7):
        fwd_x[q].wait_recv()

    def cut(n):
        return pl.ds(n * (seq // CUTS), seq // CUTS)

    def rows_of(chip_x, chip_y, core, k):
        return ((2 * (1 - chip_x) + core) * IMGS + OWN * chip_y + k) * seq

    def lent(chip_y, k, n):
        return pl.ds(pl.multiple_of(rows_of(1 - x, chip_y, c, k) + n * (seq // CUTS), seq // CUTS), seq // CUTS)

    def part0(k, n, chip_y):
        return remote(hid.at[k, cut(n), :], out.at[lent(chip_y, k, n), :], s_p0.at[k], r_p0.at[k, n], yp)

    def give0(k, n):
        return remote(out.at[lent(y, k, n), :], x1.at[k, cut(n), :], s_g0.at[k], r_g0.at[k, n], xp)

    def part1(k, n, chip_x):
        rows = pl.ds(pl.multiple_of(rows_of(chip_x, y, c, k) + n * (seq // CUTS), seq // CUTS), seq // CUTS)
        return remote(hid.at[OWN + k, cut(n), :], out.at[rows, :], s_p1, r_p1.at[k, n], xp)

    def near(k, n):
        part0(k, n, y).wait_recv()
        rows = lent(y, k, n)
        out[rows, :] = (acc[OWN + k, cut(n), :] + out[rows, :].astype(F32)).astype(BF16)
        give0(k, n).start()

    @pl.loop(0, OWN)
    def _(k):
        @pl.loop(0, 2)
        def _(mine):
            i = k + OWN * mine

            @pl.when(i == 0)
            def _():
                acc[i] += mlp_part(i, 3, 0, SPLIT, mlp)

            @pl.when(i > 0)
            def _():
                acc[i] += mlp_part(i, 2, 0, SPLIT, mlp) + mlp_part(i, 3, 0, SPLIT, mlp)

            @pl.when(mine == 0)
            def _():
                hid[k] = acc[k].astype(BF16)
                for n in range(CUTS):
                    part0(k, n, 1 - y).start()

        @pl.when(k == 0)
        def _():
            for q in (6, 7):
                nxt_y[q].wait_recv()
                fwd_y[q].start()

        @pl.when(k >= 1)
        def _():
            near(0, k - 1)

    sent(s_f0, BLOCK)
    for q in range(PIECES):
        nxt_load(2, q).start()
    filled(r_f1, BLOCK)
    for q in range(PIECES):
        nxt_load(3, q).start()

    def part_of(chip_x, chip_y, core, k, n):
        return out.at[pl.ds(rows_of(chip_x, chip_y, core, k) + n * (seq // PARTS), seq // PARTS), :]

    def image_at(chip_x, chip_y, core, k):
        return out.at[pl.ds(rows_of(chip_x, chip_y, core, k), seq), :]

    def put_core(k):
        ref = image_at(x, y, c, k)
        return remote(ref, ref, s_oc, r_oc, cp)

    def pass_y(k):
        ref = image_at(x, 1 - y, c, k)
        return remote(ref, ref, s_ey, r_ey, cp)

    def put(k, n):
        ref = part_of(x, y, c, k, n)
        return (
            remote(ref, ref, s_oy, r_oy.at[k, n], yp),
            remote(ref, ref, s_ox, r_ox.at[k, n], xp),
        )

    def pass_on(k, n):
        of_x = part_of(1 - x, y, c, k, n)
        of_y = part_of(x, 1 - y, c, k, n)
        of_d = part_of(1 - x, 1 - y, c, k, n)
        return (
            remote(of_x, of_x, s_od, r_od.at[k, n], yp),
            remote(of_y, of_y, s_od, r_od.at[k, n], xp),
            remote(of_x, of_x, s_ex, r_ex, cp),
            remote(of_d, of_d, s_ed, r_ed, cp),
        )

    def come(k, n):
        def into(ref, recv):
            return remote(ref, ref, s_ox, recv.at[k, n], cp)

        return (
            into(part_of(1 - x, y, c, k, n), r_ox),
            into(part_of(x, 1 - y, c, k, n), r_oy),
            into(part_of(1 - x, 1 - y, c, k, n), r_od),
        )

    def start_part1(k):
        sent(s_g0.at[k], seq)
        for n in range(CUTS):
            part1(k, n, 1 - x).start()

    def finish_piece(k, n):
        part1(k, n, x).wait_recv()
        rows = pl.ds(pl.multiple_of(rows_of(x, y, c, k) + n * (seq // CUTS), seq // CUTS), seq // CUTS)
        out[rows, :] = (acc[k, cut(n), :] + out[rows, :].astype(F32)).astype(BF16)
        for copy in put(k, n):
            copy.start()

    def finish(k, first=0):
        for n in range(first, CUTS):
            finish_piece(k, n)
        put_core(k).start()

    def pass_x(k, n):
        come(k, n)[0].wait_recv()
        to_d, _, x_core, _ = pass_on(k, n)

        @pl.when(k * PARTS + n < TURN)
        def _():
            to_d.start()

        x_core.start()

    def pass_x_all(k):
        for n in range(PARTS):
            pass_x(k, n)

    near(0, CUTS - 1)
    sent(s_p0.at[0], seq)
    for slot in range(4):
        filled(loc1.at[slot], BLOCK)

    @pl.loop(0, 2 * OWN)
    def _(t):
        theirs = (t == 2) | (t == 4) | (t >= 6)
        k_own, k_their = (t + 1) // 2, (t - 1) // 2

        @pl.when(jnp.logical_not(theirs))
        def _():
            values = out[pl.ds(pl.multiple_of(rows_of(1 - x, y, c, k_own), seq), seq), :].astype(F32)
            hid[0] = (normalize(values) * row(ln, 1)).astype(BF16)
            acc[0] = jnp.zeros((seq, dim), F32)

        @pl.when(theirs)
        def _():
            for n in range(CUTS):
                give0(k_their, n).wait_recv()
            values = x1[k_their].astype(F32)
            hid[0] = (normalize(values) * row(ln, 1)).astype(BF16)
            acc[k_their] = values + row(bo, 1) + row(b2, 1)

        where = jnp.where(theirs, k_their, 0)

        @pl.loop(0, 4)
        def _(slot):
            acc[where] += both(0, slot, 1)

            @pl.when((t <= 1) & (slot != 1))
            def _():
                near(t + 1, slot // 2 + slot // 3)

            @pl.when((t == 7) & (slot % 2 == 1))
            def _():
                finish_piece(2, slot // 2)

        @pl.when(jnp.logical_not(theirs))
        def _():
            hid[OWN + k_own] = acc[0].astype(BF16)

        @pl.when(t <= 1)
        def _():
            near(t + 1, CUTS - 1)
            start_part1(t)

        @pl.when((t == 2) | (t == 4))
        def _():
            finish(k_their)

        @pl.when(t == 4)
        def _():
            for n in range(CUTS):
                near(OWN - 1, n)
            start_part1(2)

        @pl.when(t == 5)
        def _():
            pass_x_all(0)

        @pl.when(t == 6)
        def _():
            pass_x_all(1)
            start_part1(3)

    finish(2, 2)
    finish(3)

    for copy in biases:
        copy.wait_send()
    for sem in (s_c0, s_x0, s_c1, s_y1, s_f1):
        sent(sem, BLOCK)
    for k in range(1, OWN):
        sent(s_p0.at[k], seq)
    sent(s_p1, OWN * seq)

    early, lag = 2, 6
    total = OWN * PARTS

    @pl.loop(0, total + lag)
    def _(j):
        @pl.when(j < total)
        def _():
            k, n = j // PARTS, j % PARTS
            come(k, n)[1].wait_recv()

            @pl.when(j >= TURN)
            def _():
                pass_on(k, n)[1].start()

            @pl.when(n == PARTS - 1)
            def _():
                pass_y(k).start()

        @pl.when((j >= early * PARTS) & (j < total))
        def _():
            pass_x(j // PARTS, j % PARTS)

        @pl.when(j >= lag)
        def _():
            k, n = (j - lag) // PARTS, (j - lag) % PARTS
            come(k, n)[2].wait_recv()
            pass_on(k, n)[3].start()

    for sem in (s_oc, s_ey, s_ox, s_oy, s_od, s_ex, s_ed, r_oc, r_ey, r_ex, r_ed):
        sent(sem, OWN * seq)


def solution(mesh):
    col_spec = P(None, None, "tp")
    row_spec = P(None, "tp", None)
    in_specs = (P("dp", None, None), P(), col_spec, col_spec, col_spec, P(), P(), row_spec, P(), col_spec, P(None, "tp"), row_spec, P())

    def per_device(tokens_in, ln_scale, w_query, w_key, w_value, q_scale, k_scale, w_out, b_out, w_up, b_up, w_down, b_down):
        n_images, seq, dim = tokens_in.shape
        layers, _, heads_w = w_query.shape
        mlp = w_up.shape[2]
        across = lambda w: jnp.swapaxes(w, 1, 2)
        any_spec = pl.BlockSpec(memory_space=pl.ANY)
        vm_spec = pl.BlockSpec(memory_space=pltpu.VMEM)
        dma = lambda *shape: pltpu.SemaphoreType.DMA(shape)
        one = pltpu.SemaphoreType.DMA
        shape = jax.ShapeDtypeStruct
        encoded, *_ = pl.pallas_call(
            fused,
            out_shape=(
                pltpu.VMEM((n_images * seq, dim), BF16),
                shape((3, 3 * heads_w, dim), BF16),
                shape((3, heads_w, dim), BF16),
                shape((3, dim, mlp), BF16),
                shape((3, mlp, dim), BF16),
            ),
            in_specs=[any_spec] * 13,
            out_specs=(vm_spec,) + (any_spec,) * 4,
            scratch_shapes=[
                pltpu.VMEM((4, 3 * heads_w, dim), BF16),
                pltpu.VMEM((4, heads_w, dim), BF16),
                pltpu.VMEM((4, dim, mlp), BF16),
                pltpu.VMEM((4, mlp, dim), BF16),
                pltpu.VMEM((6, layers, mlp), BF16),
                *[pltpu.VMEM(v.shape, BF16) for v in (ln_scale, q_scale, k_scale, b_out, b_down)],
                pltpu.VMEM((layers, 2, q_scale.shape[1], seq), F32),
                pltpu.VMEM((IMGS, seq, dim), F32),
                pltpu.VMEM((IMGS, seq, dim), BF16),
                pltpu.VMEM((OWN, seq, dim), BF16),
                dma(6),
                one, dma(4), dma(IMGS), dma(5), dma(5),
                one, one, *[one, dma(PIECES)] * 2,
                one, one, one, dma(PIECES), one, one,
                *[dma(OWN), dma(OWN, CUTS)] * 2, one, dma(OWN, CUTS),
                *[one] * 4,
                *[one, dma(OWN, PARTS)] * 3,
                *[one] * 4,
            ],
            compiler_params=pltpu.CompilerParams(
                collective_id=0, has_side_effects=True, vmem_limit_bytes=45500000),
        )(tokens_in.reshape(n_images * seq, dim), across(w_query), across(w_key), across(w_value), w_out, w_up, w_down, b_up, ln_scale, q_scale, k_scale, b_out, b_down)
        return encoded.reshape(n_images, seq, dim)

    return jax.shard_map(per_device, mesh=mesh, in_specs=in_specs, out_specs=P("dp", None, None), check_vma=False)
```
